16 devices in a mesh: dp: 4 (over z, y), sp: 4 (over x, core).
Axes of the slice: x: 2, y: 2, z: 2, core: 2. Of those that a mesh axis runs over, the one named last changes fastest.
Arguments:
- resid_x: bfloat16 [48, 512, 5120], P('dp', 'sp'), parts along dimension 0
- positions: int32 [48, 512], P('dp', 'sp'), parts along dimension 0
- w_query: bfloat16 [5120, 5120], replicated
- w_key: bfloat16 [5120, 5120], replicated
- w_value: bfloat16 [5120, 5120], replicated
- w_out: bfloat16 [5120, 5120], replicated
- gain_q: bfloat16 [5120], replicated
- gain_k: bfloat16 [5120], replicated
- gain_out: bfloat16 [5120], replicated
Outputs:
- output: bfloat16 [48, 512, 5120], P('dp', 'sp'), parts along dimension 0
There are 4 independent parts. The reference program is written for one: setup_inputs(seed, part) draws one part's arguments, and reference() takes and returns one part's arrays. A program takes and returns all parts, laid end to end along the dimension named above; an argument that names none is the same for every part.
All inputs are finite; a program needn't handle non-finite values.
Results may differ from the reference program's by a relative error of at most 0.0172881.
Values are sent between devices in bfloat16 or wider.
A program may use at most 1 GiB of HBM per device.

```python
import jax
import jax.numpy as jnp
from jax import lax

BATCH = 12
SEQ = 512
D_MODEL = 5120
HEADS = 40
HEAD_DIM = 128
DOC_LEN = 512
QUERY_BLOCKS = 8
ROPE_THETA = 500000.0
NORM_EPS = 1e-6
SCALE = HEAD_DIM ** -0.5


def setup_inputs(seed: int = 0, part: int = 0) -> dict:
    base_key = jax.random.key(seed)
    shared_keys = jax.random.split(base_key, 8)
    part_keys = jax.random.split(jax.random.fold_in(shared_keys[7], part), 2)
    resid_x = jax.random.normal(part_keys[0], (BATCH, SEQ, D_MODEL), jnp.float32).astype(jnp.bfloat16)
    token_idx = jnp.arange(SEQ, dtype=jnp.int32)[None, :]
    starts = jax.random.randint(part_keys[1], (BATCH, SEQ), 0, DOC_LEN) == 0
    starts = jnp.logical_or(starts, token_idx == 0)
    last_start = lax.cummax(jnp.where(starts, token_idx, 0), axis=1)
    positions = (token_idx - last_start).astype(jnp.int32)
    w_scale = D_MODEL ** -0.5
    matrices = [(jax.random.normal(shared_keys[w_idx], (D_MODEL, D_MODEL), jnp.float32) * w_scale).astype(jnp.bfloat16) for w_idx in range(4)]
    gains = [(0.5 + jax.random.normal(shared_keys[4 + g_idx], (D_MODEL,), jnp.float32)).astype(jnp.bfloat16) for g_idx in range(3)]
    return {'resid_x': resid_x, 'positions': positions, 'w_query': matrices[0], 'w_key': matrices[1], 'w_value': matrices[2], 'w_out': matrices[3], 'gain_q': gains[0], 'gain_k': gains[1], 'gain_out': gains[2]}


def rope_tables(pos_ids):
    inv_freq = 1.0 / (ROPE_THETA ** (jnp.arange(0, HEAD_DIM, 2, dtype=jnp.float32) / HEAD_DIM))
    angles = pos_ids.astype(jnp.float32)[..., None] * inv_freq
    return jnp.cos(angles), jnp.sin(angles)


def apply_rope(heads_f32, cos_t, sin_t):
    half = HEAD_DIM // 2
    cos_b = cos_t[:, :, None, :]
    sin_b = sin_t[:, :, None, :]
    first = heads_f32[..., :half]
    second = heads_f32[..., half:]
    return jnp.concatenate([first * cos_b - second * sin_b, second * cos_b + first * sin_b], axis=-1)


def rms_scale(vals_f32, gain):
    mean_sq = jnp.mean(vals_f32 * vals_f32, axis=-1, keepdims=True)
    return vals_f32 * lax.rsqrt(mean_sq + NORM_EPS) * gain.astype(jnp.float32)


def norm_rope(x_rows, weight, gain, cos_t, sin_t):
    proj = jnp.dot(x_rows, weight, preferred_element_type=jnp.float32).astype(jnp.bfloat16).astype(jnp.float32)
    normed = rms_scale(proj, gain).reshape(BATCH, SEQ, HEADS, HEAD_DIM)
    return apply_rope(normed, cos_t, sin_t).astype(jnp.bfloat16)


def head_attention(operands):
    q_head, k_head, v_head = operands
    block = SEQ // QUERY_BLOCKS
    q_blocks = q_head.reshape(BATCH, QUERY_BLOCKS, block, HEAD_DIM).transpose(1, 0, 2, 3)
    k_f32 = k_head.astype(jnp.float32)
    v_f32 = v_head.astype(jnp.float32)
    key_idx = jnp.arange(SEQ)

    def one_block(blk_ops):
        q_blk, blk_idx = blk_ops
        scores = jnp.einsum('bqd,bkd->bqk', q_blk.astype(jnp.float32), k_f32) * SCALE
        q_idx = blk_idx * block + jnp.arange(block)
        mask = key_idx[None, :] <= q_idx[:, None]
        scores = jnp.where(mask[None], scores, -1e30)
        probs = jax.nn.softmax(scores, axis=-1).astype(jnp.bfloat16).astype(jnp.float32)
        return jnp.einsum('bqk,bkd->bqd', probs, v_f32).astype(jnp.bfloat16)

    out_blocks = lax.map(one_block, (q_blocks, jnp.arange(QUERY_BLOCKS)))
    return out_blocks.transpose(1, 0, 2, 3).reshape(BATCH, SEQ, HEAD_DIM)


def reference(resid_x, positions, w_query, w_key, w_value, w_out, gain_q, gain_k, gain_out):
    cos_t, sin_t = rope_tables(positions)
    x_rows = resid_x.reshape(BATCH * SEQ, D_MODEL)
    q_all = norm_rope(x_rows, w_query, gain_q, cos_t, sin_t)
    k_all = norm_rope(x_rows, w_key, gain_k, cos_t, sin_t)
    v_all = jnp.dot(x_rows, w_value, preferred_element_type=jnp.float32).astype(jnp.bfloat16).reshape(BATCH, SEQ, HEADS, HEAD_DIM)
    per_head = lax.map(head_attention, (q_all.transpose(2, 0, 1, 3), k_all.transpose(2, 0, 1, 3), v_all.transpose(2, 0, 1, 3)))
    attn_rows = per_head.transpose(1, 2, 0, 3).reshape(BATCH * SEQ, D_MODEL)
    attn_out = jnp.dot(attn_rows, w_out, preferred_element_type=jnp.float32).astype(jnp.bfloat16).astype(jnp.float32)
    y_rows = x_rows.astype(jnp.float32) + rms_scale(attn_out, gain_out)
    return y_rows.astype(jnp.bfloat16).reshape(BATCH, SEQ, D_MODEL)
```

```python
import functools

import jax
import jax.numpy as jnp
from jax import lax
from jax.experimental import pallas as pl
from jax.experimental.pallas import tpu as pltpu
from jax.sharding import PartitionSpec as P

HEAD_DIM = 128
ROPE_THETA = 500000.0
NORM_EPS = 1e-6
SCALE = HEAD_DIM ** -0.5
LOG2E = 1.4426950408889634
TILE_N = 512
HEADS_PER_STEP = 4
VMEM_BYTES = 63 * 2 ** 20


def rope_tables(pos_ids):
    inv_freq = 1.0 / (ROPE_THETA ** (jnp.arange(0, HEAD_DIM, 2, dtype=jnp.float32) / HEAD_DIM))
    angles = pos_ids.astype(jnp.float32)[..., None] * inv_freq
    cos_t, sin_t = jnp.cos(angles), jnp.sin(angles)
    return jnp.concatenate([cos_t, cos_t], axis=-1), jnp.concatenate([-sin_t, sin_t], axis=-1)


def lane_sums(sq):
    part = sq[:, :128]
    for col in range(1, sq.shape[1] // 128):
        part = part + sq[:, col * 128:(col + 1) * 128]
    return part


def load_rows(pieces, dst, sem):
    copies, row = [], 0
    for idx, (src, count) in enumerate(pieces):
        for b in range(count):
            copies.append(pltpu.make_async_copy(src.at[b], dst.at[pl.ds(row, 128), :], sem.at[len(copies)]))
            row += 128
    for cp in copies:
        cp.start()
    return copies


def qkv_kernel(n_tiles, own, counts, *refs):
    n_pieces = len(counts)
    x_hbm = refs[:n_pieces]
    wq, wk, wv, _, q_out, k_out, v_out, ssq, ssk, x_buf, sem = refs[n_pieces:]
    step = pl.program_id(0)

    @pl.when(step == 0)
    def _():
        pieces = []
        for idx, (ref, count) in enumerate(zip(x_hbm, counts)):
            if own and idx == 0:
                ref = ref.at[pl.ds(lax.axis_index('sp') * count, count)]
            pieces.append((ref, count))
        for cp in load_rows(pieces, x_buf, sem):
            cp.wait()

    def project(w_ref, out_ref, stat_ref, first):
        proj = jnp.dot(x_buf[...], w_ref[...], preferred_element_type=jnp.float32).astype(jnp.bfloat16)
        out_ref[...] = proj
        if stat_ref is None:
            return
        wide = proj.astype(jnp.float32)
        part = lane_sums(wide * wide)

        @pl.when(step == first)
        def _():
            stat_ref[...] = part

        @pl.when(step != first)
        def _():
            stat_ref[...] = stat_ref[...] + part

    @pl.when(step < n_tiles)
    def _():
        project(wq, q_out, ssq, 0)

    @pl.when((step >= n_tiles) & (step < 2 * n_tiles))
    def _():
        project(wk, k_out, ssk, n_tiles)

    @pl.when(step >= 2 * n_tiles)
    def _():
        project(wv, v_out, None, 0)


def qkv_call(pieces, counts, own, w_query, w_key, w_value, after, name):
    width = w_query.shape[0]
    n_tiles = width // TILE_N
    rows = sum(counts) * 128

    def tile_map(which):
        return lambda step: (0, jnp.clip(step - which * n_tiles, 0, n_tiles - 1))

    outs = pl.pallas_call(
        functools.partial(qkv_kernel, n_tiles, own, counts),
        grid=(3 * n_tiles,),
        in_specs=[pl.BlockSpec(memory_space=pl.ANY)] * len(pieces)
        + [pl.BlockSpec((width, TILE_N), tile_map(which)) for which in range(3)]
        + [pl.BlockSpec(memory_space=pl.ANY)],
        out_specs=[pl.BlockSpec((rows, TILE_N), tile_map(which)) for which in range(3)]
        + [pl.BlockSpec((rows, 128), lambda step: (0, 0))] * 2,
        out_shape=[jax.ShapeDtypeStruct((rows, width), jnp.bfloat16)] * 3
        + [jax.ShapeDtypeStruct((rows, 128), jnp.float32)] * 2,
        scratch_shapes=[pltpu.VMEM((rows, width), jnp.bfloat16), pltpu.SemaphoreType.DMA((sum(counts),))],
        compiler_params=pltpu.CompilerParams(vmem_limit_bytes=VMEM_BYTES, dimension_semantics=("arbitrary",)),
        cost_estimate=pl.CostEstimate(flops=6 * rows * width * width, transcendentals=0, bytes_accessed=6 * width * width),
        name=name,
    )(*pieces, w_query, w_key, w_value, after)
    n_batch = sum(counts) // 2
    q, k, v = (o.reshape(2, n_batch, 128, width) for o in outs[:3])
    ssq, ssk = (o.reshape(2, n_batch, 128, 128) for o in outs[3:])
    return q, k, v, ssq, ssk


def attention_kernel(width, near_refs, far_refs, cos_ref, sin_ref, gq_ref, gk_ref, on_ref, of_ref, scratch):
    dev = lax.axis_index('sp')
    chip, core = dev // 2, dev % 2
    groups = ((near_refs, chip), (far_refs, 1 - chip))
    inv = {}
    for g_idx, (refs, half) in enumerate(groups):
        for stat in (3, 4):
            for r in range(2):
                total = jnp.sum(refs[stat][r, 0], axis=-1, keepdims=True)
                inv[g_idx, stat, r] = lax.rsqrt(total * (1.0 / width) + NORM_EPS)
    row_id = lax.broadcasted_iota(jnp.int32, (256, 256), 0)
    col_id = lax.broadcasted_iota(jnp.int32, (256, 256), 1)
    causal = col_id <= row_id
    factor = SCALE * LOG2E

    def scores(q, k):
        return lax.dot_general(q, k, (((1,), (1,)), ((), ())), preferred_element_type=jnp.float32)

    for h in range(HEADS_PER_STEP):
        q_s, k_s, v_s, o_s = scratch[4 * h:4 * h + 4]
        lanes = slice(h * 128, (h + 1) * 128)
        gains = (gq_ref[:, lanes].astype(jnp.float32), gk_ref[:, lanes].astype(jnp.float32))
        for g_idx, (refs, half) in enumerate(groups):
            for r in range(2):
                slot = core if r == 0 else 1 - core
                rows = pl.ds(pl.multiple_of((half * 2 + slot) * 128, 128), 128)
                cos_v = cos_ref[0, rows, :]
                sin_v = sin_ref[0, rows, :]
                for which, dst in ((0, q_s), (1, k_s)):
                    u = refs[which][r, 0, :, lanes].astype(jnp.float32)
                    u = u * inv[g_idx, 3 + which, r] * gains[which]
                    rot = u * cos_v + pltpu.roll(u, 64, 1) * sin_v
                    dst[half, pl.ds(pl.multiple_of(slot * 128, 128), 128), :] = rot.astype(jnp.bfloat16)
                v_s[half, pl.ds(pl.multiple_of(slot * 128, 128), 128), :] = refs[2][r, 0, :, lanes]

        q_a, q_b, k_a, k_b, v_a, v_b = q_s[0], q_s[1], k_s[0], k_s[1], v_s[0], v_s[1]
        s_a = jnp.where(causal, scores(q_a, k_a), -1e30)
        m_a = jnp.max(s_a, axis=-1, keepdims=True) * factor
        p_a = jnp.exp2(s_a * factor - m_a)
        l_a = jnp.sum(p_a, axis=-1, keepdims=True)
        p_a = (p_a * (1.0 / l_a)).astype(jnp.bfloat16)
        o_s[0] = jnp.dot(p_a, v_a, preferred_element_type=jnp.float32).astype(jnp.bfloat16)

        s_ba = scores(q_b, k_a)
        s_bb = jnp.where(causal, scores(q_b, k_b), -1e30)
        m_b = jnp.maximum(jnp.max(s_ba, axis=-1, keepdims=True), jnp.max(s_bb, axis=-1, keepdims=True)) * factor
        p_ba = jnp.exp2(s_ba * factor - m_b)
        p_bb = jnp.exp2(s_bb * factor - m_b)
        r_b = 1.0 / (jnp.sum(p_ba, axis=-1, keepdims=True) + jnp.sum(p_bb, axis=-1, keepdims=True))
        p_ba = (p_ba * r_b).astype(jnp.bfloat16)
        p_bb = (p_bb * r_b).astype(jnp.bfloat16)
        o_b = jnp.dot(p_ba, v_a, preferred_element_type=jnp.float32)
        o_b = o_b + jnp.dot(p_bb, v_b, preferred_element_type=jnp.float32)
        o_s[1] = o_b.astype(jnp.bfloat16)

        for out_ref, half in ((on_ref, chip), (of_ref, 1 - chip)):
            for r in range(2):
                slot = core if r == 0 else 1 - core
                out_ref[r, 0, :, lanes] = o_s[half, pl.ds(pl.multiple_of(slot * 128, 128), 128), :]


def attention_body(width, *refs):
    attention_kernel(width, refs[:5], refs[5:10], refs[10], refs[11], refs[12], refs[13], refs[14], refs[15], refs[16:])


def attention_call(near, far, first, n_batch, cos_t, sin_t, gain_q, gain_k, name):
    width = near[0].shape[-1]
    cols = HEADS_PER_STEP * 128

    def near_map(b, h):
        return (0, b + first, 0, h)

    def far_map(b, h):
        return (0, b, 0, h)

    def specs(index_map):
        stat_map = lambda b, h: index_map(b, 0)
        return [pl.BlockSpec((2, 1, 128, cols), index_map)] * 3 + [pl.BlockSpec((2, 1, 128, 128), stat_map)] * 2

    table_spec = pl.BlockSpec((1, 512, 128), lambda b, h: (b + first, 0, 0))
    gain_spec = pl.BlockSpec((1, cols), lambda b, h: (0, h))
    out_spec = pl.BlockSpec((2, 1, 128, cols), far_map)
    out_shape = jax.ShapeDtypeStruct((2, n_batch, 128, width), jnp.bfloat16)
    n_heads = width // 128
    return pl.pallas_call(
        functools.partial(attention_body, width),
        grid=(n_batch, width // cols),
        in_specs=specs(near_map) + specs(far_map) + [table_spec] * 2 + [gain_spec] * 2,
        out_specs=[out_spec] * 2,
        out_shape=[out_shape] * 2,
        scratch_shapes=[pltpu.VMEM((2, 256, 128), jnp.bfloat16)] * (4 * HEADS_PER_STEP),
        compiler_params=pltpu.CompilerParams(vmem_limit_bytes=VMEM_BYTES, dimension_semantics=("arbitrary", "arbitrary")),
        cost_estimate=pl.CostEstimate(flops=n_batch * n_heads * 512 * 512 * 128 * 8, transcendentals=0,
                                      bytes_accessed=n_batch * 512 * width * 8),
        name=name,
    )(*near, *far, cos_t, sin_t, gain_q.reshape(1, width), gain_k.reshape(1, width))


def out_kernel(n_tiles, o_counts, x_counts, own, *refs):
    n_o, n_x = len(o_counts), len(x_counts)
    o_hbm, x_hbm = refs[:n_o], refs[n_o:n_o + n_x]
    w_ref, gain_ref = refs[n_o + n_x:n_o + n_x + 2]
    y_hbm = refs[n_o + n_x + 3:n_o + 2 * n_x + 3]
    o_buf, x_buf, a_buf, ss_buf, o_sem, x_sem, y_sem = refs[n_o + 2 * n_x + 3:]
    step = pl.program_id(0)
    width = o_buf.shape[1]

    def at_own(ref, idx, count):
        return ref.at[pl.ds(lax.axis_index('sp') * count, count)] if own and idx == 0 else ref

    def x_copies():
        copies, row = [], 0
        for idx, count in enumerate(x_counts):
            src = at_own(x_hbm[idx], idx, count)
            for b in range(count):
                copies.append(pltpu.make_async_copy(src.at[b], x_buf.at[pl.ds(row, 128), :], x_sem.at[row // 128]))
                row += 128
        return copies

    @pl.when(step == 0)
    def _():
        copies, seen = [], 0
        total = sum(o_counts)
        for ref, count in zip(o_hbm, o_counts):
            for r in range(2):
                for b in range(count):
                    row = (r * total + seen + b) * 128
                    copies.append(pltpu.make_async_copy(ref.at[r, b], o_buf.at[pl.ds(row, 128), :], o_sem.at[row // 128]))
            seen += count
        for cp in copies:
            cp.start()
        for cp in x_copies():
            cp.start()
        for cp in copies:
            cp.wait()

    a_tile = jnp.dot(o_buf[...], w_ref[...], preferred_element_type=jnp.float32).astype(jnp.bfloat16)
    a_buf[step] = a_tile
    wide = a_tile.astype(jnp.float32)
    part = lane_sums(wide * wide)

    @pl.when(step == 0)
    def _():
        ss_buf[...] = part

    @pl.when(step != 0)
    def _():
        ss_buf[...] = ss_buf[...] + part

    @pl.when(step == n_tiles - 1)
    def _():
        for cp in x_copies():
            cp.wait()
        copies, row = [], 0
        for idx, count in enumerate(x_counts):
            dst = at_own(y_hbm[idx], idx, count)
            for b in range(count):
                rows = slice(row, row + 128)
                inv = lax.rsqrt(jnp.sum(ss_buf[rows, :], axis=-1, keepdims=True) * (1.0 / width) + NORM_EPS)
                for t in range(n_tiles):
                    cols = slice(t * TILE_N, (t + 1) * TILE_N)
                    normed = a_buf[t, rows, :].astype(jnp.float32) * inv * gain_ref[:, cols].astype(jnp.float32)
                    x_buf[rows, cols] = (x_buf[rows, cols].astype(jnp.float32) + normed).astype(jnp.bfloat16)
                cp = pltpu.make_async_copy(x_buf.at[pl.ds(row, 128), :], dst.at[b], y_sem.at[row // 128])
                cp.start()
                copies.append(cp)
                row += 128
        for cp in copies:
            cp.wait()


def out_call(o_list, x_list, x_counts, own, out_batches, w_out, gain_out, after, name):
    width = w_out.shape[0]
    n_tiles = width // TILE_N
    o_counts = tuple(o.shape[1] for o in o_list)
    rows = sum(x_counts) * 128
    any_spec = pl.BlockSpec(memory_space=pl.ANY)
    return pl.pallas_call(
        functools.partial(out_kernel, n_tiles, o_counts, x_counts, own),
        grid=(n_tiles,),
        in_specs=[any_spec] * (len(o_list) + len(x_list))
        + [pl.BlockSpec((width, TILE_N), lambda step: (0, step)), pl.BlockSpec((1, width), lambda step: (0, 0)), any_spec],
        out_specs=[any_spec] * len(x_list),
        out_shape=[jax.ShapeDtypeStruct((n, 128, width), jnp.bfloat16) for n in out_batches],
        scratch_shapes=[pltpu.VMEM((rows, width), jnp.bfloat16), pltpu.VMEM((rows, width), jnp.bfloat16),
                        pltpu.VMEM((n_tiles, rows, TILE_N), jnp.bfloat16), pltpu.VMEM((rows, 128), jnp.float32),
                        pltpu.SemaphoreType.DMA((rows // 128,)), pltpu.SemaphoreType.DMA((rows // 128,)),
                        pltpu.SemaphoreType.DMA((rows // 128,))],
        compiler_params=pltpu.CompilerParams(vmem_limit_bytes=VMEM_BYTES, dimension_semantics=("arbitrary",)),
        cost_estimate=pl.CostEstimate(flops=2 * rows * width * width, transcendentals=0, bytes_accessed=2 * width * width),
        name=name,
    )(*o_list, *x_list, w_out, gain_out.reshape(1, width), after)


def solution(mesh):
    def local_block(x_loc, pos_loc, w_query, w_key, w_value, w_out, gain_q, gain_k, gain_out):
        batch, seq_loc, width = x_loc.shape
        per_dev = batch // 4
        dev = lax.axis_index('sp')

        def swap(arr, r):
            return lax.ppermute(arr, 'sp', [(i, i ^ r) for i in range(4)])

        def piece(r, first, count):
            return lax.dynamic_slice_in_dim(x_loc, (dev ^ r) * per_dev + first, count, axis=0)

        x_far01 = [swap(piece(r, 0, 2), r) for r in (2, 3)]
        x_near = swap(piece(1, 0, per_dev), 1)
        pos_parts = [lax.dynamic_slice_in_dim(pos_loc, dev * per_dev, per_dev, axis=0)]
        for r in range(1, 4):
            pos_parts.append(swap(lax.dynamic_slice_in_dim(pos_loc, (dev ^ r) * per_dev, per_dev, axis=0), r))

        near = qkv_call([x_loc, x_near], (per_dev, per_dev), True, w_query, w_key, w_value, gain_q, "qkv_near")
        p2, p3, x_far01[0], x_far01[1] = lax.optimization_barrier((piece(2, 2, 1), piece(3, 2, 1), x_far01[0], x_far01[1]))
        x_far2 = [swap(p2, 2), swap(p3, 3)]
        far01 = qkv_call(x_far01, (2, 2), False, w_query, w_key, w_value, near[3], "qkv_far01")
        pos_parts, _ = lax.optimization_barrier((pos_parts, near[3]))
        pos_rel = jnp.stack(pos_parts)
        pos_mine = jnp.concatenate([lax.dynamic_index_in_dim(pos_rel, dev ^ j, axis=0, keepdims=False) for j in range(4)], axis=1)
        cos_t, sin_t = rope_tables(pos_mine)
        on01, of01 = attention_call(near, far01, 0, 2, cos_t, sin_t, gain_q, gain_k, "attn01")
        y_far01 = out_call([of01], x_far01, (2, 2), False, (2, 2), w_out, gain_out, gain_q, "out_far01")
        z_far01 = [swap(y_far01[0], 2), swap(y_far01[1], 3)]
        far2 = qkv_call(x_far2, (1, 1), False, w_query, w_key, w_value, y_far01[0], "qkv_far2")
        on2, of2 = attention_call(near, far2, 2, 1, cos_t, sin_t, gain_q, gain_k, "attn2")
        y_far2 = out_call([of2], x_far2, (1, 1), False, (1, 1), w_out, gain_out, gain_q, "out_far2")
        z_far2 = [swap(y_far2[0], 2), swap(y_far2[1], 3)]
        y_all, y_near = out_call([on01, on2], [x_loc, x_near], (per_dev, per_dev), True, (batch, per_dev), w_out, gain_out,
                                 y_far2[0], "out_near")
        z_near = swap(y_near, 1)

        def put(acc, part, r, first):
            return lax.dynamic_update_slice_in_dim(acc, part, (dev ^ r) * per_dev + first, axis=0)

        y_all = put(y_all, z_far01[0], 2, 0)
        y_all = put(y_all, z_far01[1], 3, 0)
        y_all = put(y_all, z_near, 1, 0)
        y_all = put(y_all, z_far2[0], 2, 2)
        y_all = put(y_all, z_far2[1], 3, 2)
        return y_all

    tok_spec = P('dp', 'sp', None)
    return jax.shard_map(local_block, mesh=mesh, in_specs=(tok_spec, P('dp', 'sp'), P(), P(), P(), P(), P(), P(), P()), out_specs=tok_spec, check_vma=False)
```

```python
import functools

import jax
import jax.numpy as jnp
from jax import lax
from jax.experimental import pallas as pl
from jax.experimental.pallas import tpu as pltpu
from jax.sharding import PartitionSpec as P


HEAD_DIM = 128
ROPE_THETA = 500000.0
NORM_EPS = 1e-6
SCALE = HEAD_DIM ** -0.5
LOG2E = 1.4426950408889634
TILE_N = 512
HEADS_PER_STEP = 4
VMEM_BYTES = 63 * 2 ** 20


def rope_tables(pos_ids):
    inv_freq = 1.0 / (ROPE_THETA ** (jnp.arange(0, HEAD_DIM, 2, dtype=jnp.float32) / HEAD_DIM))
    angles = pos_ids.astype(jnp.float32)[..., None] * inv_freq
    cos_t, sin_t = jnp.cos(angles), jnp.sin(angles)
    return jnp.concatenate([cos_t, cos_t], axis=-1), jnp.concatenate([-sin_t, sin_t], axis=-1)


def lane_sums(sq):
    part = sq[:, :128]
    for col in range(1, sq.shape[1] // 128):
        part = part + sq[:, col * 128:(col + 1) * 128]
    return part


def load_rows(pieces, dst, sem):
    copies, row = [], 0
    for src, count in pieces:
        for b in range(count):
            copies.append(pltpu.make_async_copy(src.at[b], dst.at[pl.ds(row, 128), :], sem.at[len(copies)]))
            row += 128
    for cp in copies:
        cp.start()
    return copies


def qkv_kernel(n_tiles, own, counts, *refs):
    n_pieces = len(counts)
    x_hbm = refs[:n_pieces]
    wq, wk, wv, _, q_out, k_out, v_out, ssq, ssk, x_buf, sem = refs[n_pieces:]
    step = pl.program_id(0)

    @pl.when(step == 0)
    def _():
        pieces = []
        for idx, (ref, count) in enumerate(zip(x_hbm, counts)):
            if own and idx == 0:
                ref = ref.at[pl.ds(lax.axis_index('sp') * count, count)]
            pieces.append((ref, count))
        for cp in load_rows(pieces, x_buf, sem):
            cp.wait()

    def project(w_ref, out_ref, stat_ref, first):
        proj = jnp.dot(x_buf[...], w_ref[...], preferred_element_type=jnp.float32).astype(jnp.bfloat16)
        out_ref[...] = proj
        if stat_ref is None:
            return
        wide = proj.astype(jnp.float32)
        part = lane_sums(wide * wide)

        @pl.when(step == first)
        def _():
            stat_ref[...] = part

        @pl.when(step != first)
        def _():
            stat_ref[...] = stat_ref[...] + part

    @pl.when(step < n_tiles)
    def _():
        project(wq, q_out, ssq, 0)

    @pl.when((step >= n_tiles) & (step < 2 * n_tiles))
    def _():
        project(wk, k_out, ssk, n_tiles)

    @pl.when(step >= 2 * n_tiles)
    def _():
        project(wv, v_out, None, 0)


def qkv_call(pieces, counts, own, w_query, w_key, w_value, after):
    width = w_query.shape[0]
    n_tiles = width // TILE_N
    rows = sum(counts) * 128

    def tile_map(which):
        return lambda step: (0, jnp.clip(step - which * n_tiles, 0, n_tiles - 1))

    outs = pl.pallas_call(
        functools.partial(qkv_kernel, n_tiles, own, counts),
        grid=(3 * n_tiles,),
        in_specs=[pl.BlockSpec(memory_space=pl.ANY)] * len(pieces)
        + [pl.BlockSpec((width, TILE_N), tile_map(which)) for which in range(3)]
        + [pl.BlockSpec(memory_space=pl.ANY)],
        out_specs=[pl.BlockSpec((rows, TILE_N), tile_map(which)) for which in range(3)]
        + [pl.BlockSpec((rows, 128), lambda step: (0, 0))] * 2,
        out_shape=[jax.ShapeDtypeStruct((rows, width), jnp.bfloat16)] * 3
        + [jax.ShapeDtypeStruct((rows, 128), jnp.float32)] * 2,
        scratch_shapes=[pltpu.VMEM((rows, width), jnp.bfloat16), pltpu.SemaphoreType.DMA((sum(counts),))],
        compiler_params=pltpu.CompilerParams(vmem_limit_bytes=VMEM_BYTES, dimension_semantics=("arbitrary",)),
        cost_estimate=pl.CostEstimate(flops=6 * rows * width * width, transcendentals=0, bytes_accessed=6 * width * width),
    )(*pieces, w_query, w_key, w_value, after)
    n_batch = sum(counts) // 2
    q, k, v = (o.reshape(2, n_batch, 128, width) for o in outs[:3])
    ssq, ssk = (o.reshape(2, n_batch, 128, 128) for o in outs[3:])
    return q, k, v, ssq, ssk


def attention_kernel(width, near_refs, far_refs, cos_ref, sin_ref, gq_ref, gk_ref, on_ref, of_ref, scratch):
    dev = lax.axis_index('sp')
    chip, core = dev // 2, dev % 2
    groups = ((near_refs, chip), (far_refs, 1 - chip))
    inv = {}
    for g_idx, (refs, half) in enumerate(groups):
        for stat in (3, 4):
            for r in range(2):
                total = jnp.sum(refs[stat][r, 0], axis=-1, keepdims=True)
                inv[g_idx, stat, r] = lax.rsqrt(total * (1.0 / width) + NORM_EPS)
    row_id = lax.broadcasted_iota(jnp.int32, (256, 256), 0)
    col_id = lax.broadcasted_iota(jnp.int32, (256, 256), 1)
    causal = col_id <= row_id
    factor = SCALE * LOG2E

    def scores(q, k):
        return lax.dot_general(q, k, (((1,), (1,)), ((), ())), preferred_element_type=jnp.float32)

    for h in range(HEADS_PER_STEP):
        q_s, k_s, v_s, o_s = scratch[4 * h:4 * h + 4]
        lanes = slice(h * 128, (h + 1) * 128)
        gains = (gq_ref[:, lanes].astype(jnp.float32), gk_ref[:, lanes].astype(jnp.float32))
        for g_idx, (refs, half) in enumerate(groups):
            for r in range(2):
                slot = core if r == 0 else 1 - core
                rows = pl.ds(pl.multiple_of((half * 2 + slot) * 128, 128), 128)
                cos_v = cos_ref[0, rows, :]
                sin_v = sin_ref[0, rows, :]
                for which, dst in ((0, q_s), (1, k_s)):
                    u = refs[which][r, 0, :, lanes].astype(jnp.float32)
                    u = u * inv[g_idx, 3 + which, r] * gains[which]
                    rot = u * cos_v + pltpu.roll(u, 64, 1) * sin_v
                    dst[half, pl.ds(pl.multiple_of(slot * 128, 128), 128), :] = rot.astype(jnp.bfloat16)
                v_s[half, pl.ds(pl.multiple_of(slot * 128, 128), 128), :] = refs[2][r, 0, :, lanes]

        q_a, q_b, k_a, k_b, v_a, v_b = q_s[0], q_s[1], k_s[0], k_s[1], v_s[0], v_s[1]
        s_a = jnp.where(causal, scores(q_a, k_a), -1e30)
        m_a = jnp.max(s_a, axis=-1, keepdims=True) * factor
        p_a = jnp.exp2(s_a * factor - m_a)
        l_a = jnp.sum(p_a, axis=-1, keepdims=True)
        p_a = (p_a * (1.0 / l_a)).astype(jnp.bfloat16)
        o_s[0] = jnp.dot(p_a, v_a, preferred_element_type=jnp.float32).astype(jnp.bfloat16)

        s_ba = scores(q_b, k_a)
        s_bb = jnp.where(causal, scores(q_b, k_b), -1e30)
        m_b = jnp.maximum(jnp.max(s_ba, axis=-1, keepdims=True), jnp.max(s_bb, axis=-1, keepdims=True)) * factor
        p_ba = jnp.exp2(s_ba * factor - m_b)
        p_bb = jnp.exp2(s_bb * factor - m_b)
        r_b = 1.0 / (jnp.sum(p_ba, axis=-1, keepdims=True) + jnp.sum(p_bb, axis=-1, keepdims=True))
        p_ba = (p_ba * r_b).astype(jnp.bfloat16)
        p_bb = (p_bb * r_b).astype(jnp.bfloat16)
        o_b = jnp.dot(p_ba, v_a, preferred_element_type=jnp.float32)
        o_b = o_b + jnp.dot(p_bb, v_b, preferred_element_type=jnp.float32)
        o_s[1] = o_b.astype(jnp.bfloat16)

        for out_ref, half in ((on_ref, chip), (of_ref, 1 - chip)):
            for r in range(2):
                slot = core if r == 0 else 1 - core
                out_ref[r, 0, :, lanes] = o_s[half, pl.ds(pl.multiple_of(slot * 128, 128), 128), :]


def attention_body(width, *refs):
    attention_kernel(width, refs[:5], refs[5:10], refs[10], refs[11], refs[12], refs[13], refs[14], refs[15], refs[16:])


def attention_call(near, far, first, n_batch, cos_t, sin_t, gain_q, gain_k):
    width = near[0].shape[-1]
    cols = HEADS_PER_STEP * 128

    def near_map(b, h):
        return (0, b + first, 0, h)

    def far_map(b, h):
        return (0, b, 0, h)

    def specs(index_map):
        stat_map = lambda b, h: index_map(b, 0)
        return [pl.BlockSpec((2, 1, 128, cols), index_map)] * 3 + [pl.BlockSpec((2, 1, 128, 128), stat_map)] * 2

    table_spec = pl.BlockSpec((1, 512, 128), lambda b, h: (b + first, 0, 0))
    gain_spec = pl.BlockSpec((1, cols), lambda b, h: (0, h))
    out_spec = pl.BlockSpec((2, 1, 128, cols), far_map)
    out_shape = jax.ShapeDtypeStruct((2, n_batch, 128, width), jnp.bfloat16)
    n_heads = width // 128
    return pl.pallas_call(
        functools.partial(attention_body, width),
        grid=(n_batch, width // cols),
        in_specs=specs(near_map) + specs(far_map) + [table_spec] * 2 + [gain_spec] * 2,
        out_specs=[out_spec] * 2,
        out_shape=[out_shape] * 2,
        scratch_shapes=[pltpu.VMEM((2, 256, 128), jnp.bfloat16)] * (4 * HEADS_PER_STEP),
        compiler_params=pltpu.CompilerParams(vmem_limit_bytes=VMEM_BYTES, dimension_semantics=("arbitrary", "arbitrary")),
        cost_estimate=pl.CostEstimate(flops=n_batch * n_heads * 512 * 512 * 128 * 8, transcendentals=0,
                                      bytes_accessed=n_batch * 512 * width * 8),
    )(*near, *far, cos_t, sin_t, gain_q.reshape(1, width), gain_k.reshape(1, width))


def out_kernel(n_tiles, o_counts, x_counts, own, *refs):
    n_o, n_x = len(o_counts), len(x_counts)
    o_hbm, x_hbm = refs[:n_o], refs[n_o:n_o + n_x]
    w_ref, gain_ref = refs[n_o + n_x:n_o + n_x + 2]
    y_hbm = refs[n_o + n_x + 3:n_o + 2 * n_x + 3]
    o_buf, x_buf, a_buf, ss_buf, o_sem, x_sem, y_sem = refs[n_o + 2 * n_x + 3:]
    step = pl.program_id(0)
    width = o_buf.shape[1]

    def at_own(ref, idx, count):
        return ref.at[pl.ds(lax.axis_index('sp') * count, count)] if own and idx == 0 else ref

    def x_copies():
        copies, row = [], 0
        for idx, count in enumerate(x_counts):
            src = at_own(x_hbm[idx], idx, count)
            for b in range(count):
                copies.append(pltpu.make_async_copy(src.at[b], x_buf.at[pl.ds(row, 128), :], x_sem.at[row // 128]))
                row += 128
        return copies

    @pl.when(step == 0)
    def _():
        copies, seen = [], 0
        total = sum(o_counts)
        for ref, count in zip(o_hbm, o_counts):
            for r in range(2):
                for b in range(count):
                    row = (r * total + seen + b) * 128
                    copies.append(pltpu.make_async_copy(ref.at[r, b], o_buf.at[pl.ds(row, 128), :], o_sem.at[row // 128]))
            seen += count
        for cp in copies:
            cp.start()
        for cp in x_copies():
            cp.start()
        for cp in copies:
            cp.wait()

    a_tile = jnp.dot(o_buf[...], w_ref[...], preferred_element_type=jnp.float32).astype(jnp.bfloat16)
    a_buf[step] = a_tile
    wide = a_tile.astype(jnp.float32)
    part = lane_sums(wide * wide)

    @pl.when(step == 0)
    def _():
        ss_buf[...] = part

    @pl.when(step != 0)
    def _():
        ss_buf[...] = ss_buf[...] + part

    @pl.when(step == n_tiles - 1)
    def _():
        for cp in x_copies():
            cp.wait()
        copies, row = [], 0
        for idx, count in enumerate(x_counts):
            dst = at_own(y_hbm[idx], idx, count)
            for b in range(count):
                rows = slice(row, row + 128)
                inv = lax.rsqrt(jnp.sum(ss_buf[rows, :], axis=-1, keepdims=True) * (1.0 / width) + NORM_EPS)
                for t in range(n_tiles):
                    cols = slice(t * TILE_N, (t + 1) * TILE_N)
                    normed = a_buf[t, rows, :].astype(jnp.float32) * inv * gain_ref[:, cols].astype(jnp.float32)
                    x_buf[rows, cols] = (x_buf[rows, cols].astype(jnp.float32) + normed).astype(jnp.bfloat16)
                cp = pltpu.make_async_copy(x_buf.at[pl.ds(row, 128), :], dst.at[b], y_sem.at[row // 128])
                cp.start()
                copies.append(cp)
                row += 128
        for cp in copies:
            cp.wait()


def out_call(o_list, x_list, x_counts, own, out_batches, w_out, gain_out, after):
    width = w_out.shape[0]
    n_tiles = width // TILE_N
    o_counts = tuple(o.shape[1] for o in o_list)
    rows = sum(x_counts) * 128
    any_spec = pl.BlockSpec(memory_space=pl.ANY)
    return pl.pallas_call(
        functools.partial(out_kernel, n_tiles, o_counts, x_counts, own),
        grid=(n_tiles,),
        in_specs=[any_spec] * (len(o_list) + len(x_list))
        + [pl.BlockSpec((width, TILE_N), lambda step: (0, step)), pl.BlockSpec((1, width), lambda step: (0, 0)), any_spec],
        out_specs=[any_spec] * len(x_list),
        out_shape=[jax.ShapeDtypeStruct((n, 128, width), jnp.bfloat16) for n in out_batches],
        scratch_shapes=[pltpu.VMEM((rows, width), jnp.bfloat16), pltpu.VMEM((rows, width), jnp.bfloat16),
                        pltpu.VMEM((n_tiles, rows, TILE_N), jnp.bfloat16), pltpu.VMEM((rows, 128), jnp.float32),
                        pltpu.SemaphoreType.DMA((rows // 128,)), pltpu.SemaphoreType.DMA((rows // 128,)),
                        pltpu.SemaphoreType.DMA((rows // 128,))],
        compiler_params=pltpu.CompilerParams(vmem_limit_bytes=VMEM_BYTES, dimension_semantics=("arbitrary",)),
        cost_estimate=pl.CostEstimate(flops=2 * rows * width * width, transcendentals=0, bytes_accessed=2 * width * width),
    )(*o_list, *x_list, w_out, gain_out.reshape(1, width), after)


def solution(mesh):
    def local_block(x_loc, pos_loc, w_query, w_key, w_value, w_out, gain_q, gain_k, gain_out):
        batch, _, _ = x_loc.shape
        per_dev = batch // 4
        dev = lax.axis_index('sp')

        def swap(arr, r):
            return lax.ppermute(arr, 'sp', [(i, i ^ r) for i in range(4)])

        def piece(r, first, count):
            return lax.dynamic_slice_in_dim(x_loc, (dev ^ r) * per_dev + first, count, axis=0)

        x_far01 = [swap(piece(r, 0, 2), r) for r in (2, 3)]
        x_near = swap(piece(1, 0, per_dev), 1)
        pos_parts = [lax.dynamic_slice_in_dim(pos_loc, dev * per_dev, per_dev, axis=0)]
        for r in range(1, 4):
            pos_parts.append(swap(lax.dynamic_slice_in_dim(pos_loc, (dev ^ r) * per_dev, per_dev, axis=0), r))

        near = qkv_call([x_loc, x_near], (per_dev, per_dev), True, w_query, w_key, w_value, gain_q)
        p2, p3, x_far01[0], x_far01[1] = lax.optimization_barrier((piece(2, 2, 1), piece(3, 2, 1), x_far01[0], x_far01[1]))
        x_far2 = [swap(p2, 2), swap(p3, 3)]
        far01 = qkv_call(x_far01, (2, 2), False, w_query, w_key, w_value, near[3])
        pos_parts, _ = lax.optimization_barrier((pos_parts, near[3]))
        pos_rel = jnp.stack(pos_parts)
        pos_mine = jnp.concatenate([lax.dynamic_index_in_dim(pos_rel, dev ^ j, axis=0, keepdims=False) for j in range(4)], axis=1)
        cos_t, sin_t = rope_tables(pos_mine)
        on01, of01 = attention_call(near, far01, 0, 2, cos_t, sin_t, gain_q, gain_k)
        y_far01 = out_call([of01], x_far01, (2, 2), False, (2, 2), w_out, gain_out, gain_q)
        z_far01 = [swap(y_far01[0], 2), swap(y_far01[1], 3)]
        far2 = qkv_call(x_far2, (1, 1), False, w_query, w_key, w_value, y_far01[0])
        on2, of2 = attention_call(near, far2, 2, 1, cos_t, sin_t, gain_q, gain_k)
        y_far2 = out_call([of2], x_far2, (1, 1), False, (1, 1), w_out, gain_out, gain_q)
        z_far2 = [swap(y_far2[0], 2), swap(y_far2[1], 3)]
        y_all, y_near = out_call([on01, on2], [x_loc, x_near], (per_dev, per_dev), True, (batch, per_dev), w_out, gain_out,
                                 y_far2[0])
        z_near = swap(y_near, 1)

        def put(acc, part, r, first):
            return lax.dynamic_update_slice_in_dim(acc, part, (dev ^ r) * per_dev + first, axis=0)

        y_all = put(y_all, z_far01[0], 2, 0)
        y_all = put(y_all, z_far01[1], 3, 0)
        y_all = put(y_all, z_near, 1, 0)
        y_all = put(y_all, z_far2[0], 2, 2)
        y_all = put(y_all, z_far2[1], 3, 2)
        return y_all

    tok_spec = P('dp', 'sp', None)

    return jax.shard_map(local_block, mesh=mesh, in_specs=(tok_spec, P('dp', 'sp'), P(), P(), P(), P(), P(), P(), P()), out_specs=tok_spec, check_vma=False)
```

```python
import functools

import jax
import jax.numpy as jnp
from jax import lax
from jax.experimental import pallas as pl
from jax.experimental.pallas import tpu as pltpu
from jax.sharding import PartitionSpec as P


HEAD_DIM = 128
ROPE_THETA = 500000.0
NORM_EPS = 1e-6
SCALE = HEAD_DIM ** -0.5
LOG2E = 1.4426950408889634
QKV_TILE = 1024
OUT_TILE = 512
HEADS_PER_STEP = 4
VMEM_BYTES = 63 * 2 ** 20


def rope_tables(pos_ids):
    inv_freq = 1.0 / (ROPE_THETA ** (jnp.arange(0, HEAD_DIM, 2, dtype=jnp.float32) / HEAD_DIM))
    angles = pos_ids.astype(jnp.float32)[..., None] * inv_freq
    cos_t, sin_t = jnp.cos(angles), jnp.sin(angles)
    return jnp.concatenate([cos_t, cos_t], axis=-1), jnp.concatenate([-sin_t, sin_t], axis=-1)


def lane_sums(sq):
    part = sq[:, :128]
    for col in range(1, sq.shape[1] // 128):
        part = part + sq[:, col * 128:(col + 1) * 128]
    return part


def row_copies(srcs, dst, sems):
    return [pltpu.make_async_copy(src, dst.at[pl.ds(i * 128, 128), :], sems.at[i]) for i, src in enumerate(srcs)]


def qkv_kernel(n_tiles, own, counts, aliased, *refs):
    n_pieces = len(counts)
    x_hbm = refs[:n_pieces]
    weights = refs[n_pieces:n_pieces + 3]
    qkv_out, stat_out, x_buf, w_buf, x_sem, w_sem = refs[n_pieces + 4 + 2 * aliased:]
    step = pl.program_id(0)
    slot = lax.rem(step, 2)

    def fetch(at_step):
        for idx, w_ref in enumerate(weights):
            @pl.when(at_step // n_tiles == idx)
            def _():
                cols = pl.ds(pl.multiple_of(lax.rem(at_step, n_tiles) * QKV_TILE, QKV_TILE), QKV_TILE)
                to = lax.rem(at_step, 2)
                pltpu.make_async_copy(w_ref.at[:, cols], w_buf.at[to], w_sem.at[to]).start()

    @pl.when(step == 0)
    def _():
        srcs = []
        for idx, (ref, count) in enumerate(zip(x_hbm, counts)):
            base = lax.axis_index('sp') * count if own and idx == 0 else 0
            srcs += [ref.at[base + b] for b in range(count)]
        copies = row_copies(srcs, x_buf, x_sem)
        for cp in copies:
            cp.start()
        fetch(step)
        for cp in copies:
            cp.wait()

    @pl.when(step + 1 < 3 * n_tiles)
    def _():
        fetch(step + 1)

    pltpu.make_async_copy(weights[0].at[:, pl.ds(0, QKV_TILE)], w_buf.at[slot], w_sem.at[slot]).wait()
    proj = jnp.dot(x_buf[...], w_buf[slot], preferred_element_type=jnp.float32).astype(jnp.bfloat16)
    qkv_out[...] = proj.reshape(qkv_out.shape)
    wide = proj.astype(jnp.float32)
    part = lane_sums(wide * wide).reshape(stat_out.shape)
    first = lax.rem(step, n_tiles) == 0

    @pl.when(first)
    def _():
        stat_out[...] = part

    @pl.when(jnp.logical_not(first))
    def _():
        stat_out[...] = stat_out[...] + part


def qkv_call(pieces, counts, own, weights, per_dev, group, batch_block, prior, after):
    width = weights[0].shape[0]
    n_tiles = width // QKV_TILE
    n_batch = sum(counts) // 2
    rows = sum(counts) * 128
    any_spec = pl.BlockSpec(memory_space=pl.ANY)
    n_in = len(pieces) + 4
    return pl.pallas_call(
        functools.partial(qkv_kernel, n_tiles, own, counts, bool(prior)),
        grid=(3 * n_tiles,),
        in_specs=[any_spec] * (n_in + len(prior)),
        out_specs=[
            pl.BlockSpec((1, 2, n_batch, 128, QKV_TILE), lambda s: (s // n_tiles, group, batch_block, 0, lax.rem(s, n_tiles))),
            pl.BlockSpec((1, 2, n_batch, 128, 128), lambda s: (s // n_tiles, group, batch_block, 0, 0))],
        out_shape=[jax.ShapeDtypeStruct((3, 4, per_dev, 128, width), jnp.bfloat16),
                   jax.ShapeDtypeStruct((3, 4, per_dev, 128, 128), jnp.float32)],
        input_output_aliases={n_in: 0, n_in + 1: 1} if prior else {},
        scratch_shapes=[pltpu.VMEM((rows, width), jnp.bfloat16), pltpu.VMEM((2, width, QKV_TILE), jnp.bfloat16),
                        pltpu.SemaphoreType.DMA((sum(counts),)), pltpu.SemaphoreType.DMA((2,))],
        compiler_params=pltpu.CompilerParams(vmem_limit_bytes=VMEM_BYTES, dimension_semantics=("arbitrary",)),
        cost_estimate=pl.CostEstimate(flops=6 * rows * width * width, transcendentals=0, bytes_accessed=6 * width * width),
    )(*pieces, *weights, after, *prior)


def attention_kernel(width, dev_ref, *refs):
    qkv_refs, stat_refs = refs[:4], refs[4:8]
    cos_ref, sin_ref, gq_ref, gk_ref, out_ref, cos_n, sin_n = refs[8:]
    dev = dev_ref[0]

    @pl.when(pl.program_id(1) == 0)
    def _():
        for which in range(2):
            for j in range(4):
                rows = slice(j * 128, (j + 1) * 128)
                total = jnp.sum(stat_refs[j][which, 0, 0], axis=-1, keepdims=True)
                inv = lax.rsqrt(total * (1.0 / width) + NORM_EPS)
                cos_n[which, rows, :] = cos_ref[0, rows, :] * inv
                sin_n[which, rows, :] = sin_ref[0, rows, :] * inv

    row_id = lax.broadcasted_iota(jnp.int32, (128, 128), 0)
    col_id = lax.broadcasted_iota(jnp.int32, (128, 128), 1)
    causal = col_id <= row_id
    factor = SCALE * LOG2E
    zeros = jnp.zeros((128, 128), jnp.bfloat16)

    def scores(q, k):
        return lax.dot_general(q, k, (((1,), (1,)), ((), ())), preferred_element_type=jnp.float32)

    def prepare(h):
        lanes = slice(h * 128, (h + 1) * 128)
        parts = ([], [])
        for which, gain_ref in ((0, gq_ref), (1, gk_ref)):
            gain = gain_ref[:, lanes].astype(jnp.float32)
            for j in range(4):
                rows = slice(j * 128, (j + 1) * 128)
                u = qkv_refs[j][which, 0, 0, :, lanes].astype(jnp.float32) * gain
                rot = u * cos_n[which, rows, :] + pltpu.roll(u, 64, 1) * sin_n[which, rows, :]
                parts[which].append(rot.astype(jnp.bfloat16))
        q, k = parts
        k_lo, k_hi = jnp.concatenate(k[:2], axis=0), jnp.concatenate(k[2:], axis=0)
        return scores(jnp.concatenate(q, axis=0), k_lo), scores(jnp.concatenate(q[2:], axis=0), k_hi)

    def finish(h, s_lo, s_hi):
        lanes = slice(h * 128, (h + 1) * 128)
        probs = []
        for j in range(4):
            blocks = []
            for c in range(j + 1):
                src, r = (s_lo, j) if c < 2 else (s_hi, j - 2)
                blk = src[r * 128:(r + 1) * 128, (c % 2) * 128:(c % 2 + 1) * 128]
                blocks.append(jnp.where(causal, blk, -1e30) if c == j else blk)
            top = functools.reduce(jnp.maximum, blocks)
            top = jnp.max(top, axis=-1, keepdims=True) * factor
            exps = [jnp.exp2(blk * factor - top) for blk in blocks]
            inv = 1.0 / jnp.sum(functools.reduce(jnp.add, exps), axis=-1, keepdims=True)
            row = [(e * inv).astype(jnp.bfloat16) for e in exps]
            probs.append(row + [zeros] * (4 - len(row)))
        p_lo = jnp.concatenate([jnp.concatenate(p[:2], axis=1) for p in probs], axis=0)
        p_hi = jnp.concatenate([jnp.concatenate(p[2:], axis=1) for p in probs[2:]], axis=0)
        v = [qkv_refs[j][2, 0, 0, :, lanes] for j in range(4)]
        o_lo = jnp.dot(p_lo, jnp.concatenate(v[:2], axis=0), preferred_element_type=jnp.float32)
        o_hi = jnp.dot(p_hi, jnp.concatenate(v[2:], axis=0), preferred_element_type=jnp.float32)
        for j in range(4):
            o = o_lo[j * 128:(j + 1) * 128]
            if j >= 2:
                o = o + o_hi[(j - 2) * 128:(j - 1) * 128]
            out_ref[jnp.bitwise_xor(dev, j), 0, :, lanes] = o.astype(jnp.bfloat16)

    ready = prepare(0)
    for h in range(HEADS_PER_STEP):
        following = prepare(h + 1) if h + 1 < HEADS_PER_STEP else None
        finish(h, *ready)
        ready = following


def attention_call(qkv, stats, dev, first, n_batch, cos_t, sin_t, gain_q, gain_k):
    width = qkv.shape[-1]
    cols = HEADS_PER_STEP * 128

    def qkv_map(j):
        return lambda b, h, dev_ref: (0, jnp.bitwise_xor(dev_ref[0], j), b + first, 0, h)

    def stat_map(j):
        return lambda b, h, dev_ref: (0, jnp.bitwise_xor(dev_ref[0], j), b + first, 0, 0)

    table_spec = pl.BlockSpec((1, 512, 128), lambda b, h, dev_ref: (b + first, 0, 0))
    gain_spec = pl.BlockSpec((1, cols), lambda b, h, dev_ref: (0, h))
    n_heads = width // 128
    return pl.pallas_call(
        functools.partial(attention_kernel, width),
        grid_spec=pltpu.PrefetchScalarGridSpec(
            num_scalar_prefetch=1,
            grid=(n_batch, width // cols),
            in_specs=[pl.BlockSpec((3, 1, 1, 128, cols), qkv_map(j)) for j in range(4)]
            + [pl.BlockSpec((2, 1, 1, 128, 128), stat_map(j)) for j in range(4)] + [table_spec] * 2 + [gain_spec] * 2,
            out_specs=pl.BlockSpec((4, 1, 128, cols), lambda b, h, dev_ref: (0, b, 0, h)),
            scratch_shapes=[pltpu.VMEM((2, 512, 128), jnp.float32)] * 2,
        ),
        out_shape=jax.ShapeDtypeStruct((4, n_batch, 128, width), jnp.bfloat16),
        compiler_params=pltpu.CompilerParams(vmem_limit_bytes=VMEM_BYTES, dimension_semantics=("arbitrary", "arbitrary")),
        cost_estimate=pl.CostEstimate(flops=n_batch * n_heads * 512 * 512 * 128 * 8, transcendentals=0,
                                      bytes_accessed=n_batch * 512 * width * 8),
    )(dev, *[qkv] * 4, *[stats] * 4, cos_t, sin_t, gain_q.reshape(1, width), gain_k.reshape(1, width))


def out_kernel(n_tiles, rel, o_counts, x_counts, own, moved, *refs):
    n_o, n_x, n_z = len(o_counts), len(x_counts), len(moved)
    pos = 0

    def take(n):
        nonlocal pos
        pos += n
        return refs[pos - n:pos]

    o_hbm, x_hbm, z_hbm = take(n_o), take(n_x), take(n_z)
    w_hbm, gain_ref, _ = take(3)
    y_hbm = take(n_x)
    o_buf, x_buf, a_buf, ss_buf, w_buf, o_sem, x_sem, y_sem, w_sem = take(9)
    z_buf, z_sem = take(2) if n_z else (None, None)
    step = pl.program_id(0)
    width = o_buf.shape[1]
    slot = lax.rem(step, 2)
    dev = lax.axis_index('sp')

    def fetch(at_step):
        cols = pl.ds(pl.multiple_of(at_step * OUT_TILE, OUT_TILE), OUT_TILE)
        to = lax.rem(at_step, 2)
        return pltpu.make_async_copy(w_hbm.at[:, cols], w_buf.at[to], w_sem.at[to])

    def at_pieces(piece_refs):
        out = []
        for idx, (ref, count) in enumerate(zip(piece_refs, x_counts)):
            base = dev * count if own and idx == 0 else 0
            out += [ref.at[base + b] for b in range(count)]
        return out

    def z_copies(outward):
        copies, i = [], 0
        for ref, (r, count, per_dev) in zip(z_hbm, moved):
            base = jnp.bitwise_xor(dev, r) * per_dev
            for b in range(count):
                src, dst = (z_buf.at[i], y_hbm[0].at[base + b]) if outward else (ref.at[b], z_buf.at[i])
                copies.append(pltpu.make_async_copy(src, dst, z_sem.at[int(outward), i]))
                i += 1
        return copies

    @pl.when(step == 0)
    def _():
        fetch(step).start()
        srcs = [ref.at[r, b] for r in rel for ref, count in zip(o_hbm, o_counts) for b in range(count)]
        copies = row_copies(srcs, o_buf, o_sem)
        for cp in copies:
            cp.start()
        for cp in copies:
            cp.wait()
        for cp in row_copies(at_pieces(x_hbm), x_buf, x_sem):
            cp.start()

    @pl.when(step + 1 < n_tiles)
    def _():
        fetch(step + 1).start()

    if n_z:
        @pl.when(step == 1)
        def _():
            for cp in z_copies(False):
                cp.start()

        @pl.when(step == 3)
        def _():
            for cp in z_copies(False):
                cp.wait()
            for cp in z_copies(True):
                cp.start()

    fetch(step).wait()
    a_tile = jnp.dot(o_buf[...], w_buf[slot], preferred_element_type=jnp.float32).astype(jnp.bfloat16)
    a_buf[step] = a_tile
    wide = a_tile.astype(jnp.float32)
    part = lane_sums(wide * wide)

    @pl.when(step == 0)
    def _():
        ss_buf[...] = part

    @pl.when(step != 0)
    def _():
        ss_buf[...] = ss_buf[...] + part

    @pl.when(step == n_tiles - 1)
    def _():
        for cp in row_copies(at_pieces(x_hbm), x_buf, x_sem):
            cp.wait()
        copies = []
        for i, dst in enumerate(at_pieces(y_hbm)):
            rows = slice(i * 128, (i + 1) * 128)
            inv = lax.rsqrt(jnp.sum(ss_buf[rows, :], axis=-1, keepdims=True) * (1.0 / width) + NORM_EPS)
            for t in range(n_tiles):
                cols = slice(t * OUT_TILE, (t + 1) * OUT_TILE)
                normed = a_buf[t, rows, :].astype(jnp.float32) * inv * gain_ref[:, cols].astype(jnp.float32)
                x_buf[rows, cols] = (x_buf[rows, cols].astype(jnp.float32) + normed).astype(jnp.bfloat16)
            cp = pltpu.make_async_copy(x_buf.at[pl.ds(i * 128, 128), :], dst, y_sem.at[i])
            cp.start()
            copies.append(cp)
        for cp in copies:
            cp.wait()
        if n_z:
            for cp in z_copies(True):
                cp.wait()


def out_call(o_list, rel, x_list, x_counts, own, out_batches, w_out, gain_out, after, z_list=(), moved=()):
    width = w_out.shape[0]
    n_tiles = width // OUT_TILE
    o_counts = tuple(o.shape[1] for o in o_list)
    rows = sum(x_counts) * 128
    any_spec = pl.BlockSpec(memory_space=pl.ANY)
    n_moved = sum(m[1] for m in moved)
    extra = [pltpu.VMEM((n_moved, 128, width), jnp.bfloat16), pltpu.SemaphoreType.DMA((2, n_moved))] if moved else []
    return pl.pallas_call(
        functools.partial(out_kernel, n_tiles, rel, o_counts, x_counts, own, moved),
        grid=(n_tiles,),
        in_specs=[any_spec] * (len(o_list) + len(x_list) + len(z_list) + 1)
        + [pl.BlockSpec((1, width), lambda step: (0, 0)), any_spec],
        out_specs=[any_spec] * len(x_list),
        out_shape=[jax.ShapeDtypeStruct((n, 128, width), jnp.bfloat16) for n in out_batches],
        scratch_shapes=[pltpu.VMEM((rows, width), jnp.bfloat16), pltpu.VMEM((rows, width), jnp.bfloat16),
                        pltpu.VMEM((n_tiles, rows, OUT_TILE), jnp.bfloat16), pltpu.VMEM((rows, 128), jnp.float32),
                        pltpu.VMEM((2, width, OUT_TILE), jnp.bfloat16)]
        + [pltpu.SemaphoreType.DMA((rows // 128,))] * 3 + [pltpu.SemaphoreType.DMA((2,))] + extra,
        compiler_params=pltpu.CompilerParams(vmem_limit_bytes=VMEM_BYTES, dimension_semantics=("arbitrary",)),
        cost_estimate=pl.CostEstimate(flops=2 * rows * width * width, transcendentals=0, bytes_accessed=2 * width * width),
    )(*o_list, *x_list, *z_list, w_out, gain_out.reshape(1, width), after)


def solution(mesh):
    def local_block(x_loc, pos_loc, w_query, w_key, w_value, w_out, gain_q, gain_k, gain_out):
        batch, _, _ = x_loc.shape
        per_dev = batch // 4
        dev = lax.axis_index('sp')

        def swap(arr, r):
            return lax.ppermute(arr, 'sp', [(i, i ^ r) for i in range(4)])

        def piece(r, first, count):
            return lax.dynamic_slice_in_dim(x_loc, (dev ^ r) * per_dev + first, count, axis=0)

        x_far01 = [swap(piece(r, 0, 2), r) for r in (2, 3)]
        x_near = swap(piece(1, 0, per_dev), 1)
        pos_parts = [lax.dynamic_slice_in_dim(pos_loc, dev * per_dev, per_dev, axis=0)]
        for r in range(1, 4):
            pos_parts.append(swap(lax.dynamic_slice_in_dim(pos_loc, (dev ^ r) * per_dev, per_dev, axis=0), r))

        weights = (w_query, w_key, w_value)
        dev_arr = jnp.full((1,), dev, jnp.int32)
        near = qkv_call([x_loc, x_near], (per_dev, per_dev), True, weights, per_dev, 0, 0, (), gain_q)
        p2, p3, x_far01[0], x_far01[1] = lax.optimization_barrier((piece(2, 2, 1), piece(3, 2, 1), x_far01[0], x_far01[1]))
        x_far2 = [swap(p2, 2), swap(p3, 3)]
        qkv01, stats01 = qkv_call(x_far01, (2, 2), False, weights, per_dev, 1, 0, near, gain_q)
        pos_parts, _ = lax.optimization_barrier((pos_parts, near[1]))
        pos_rel = jnp.stack(pos_parts)
        pos_mine = jnp.concatenate([lax.dynamic_index_in_dim(pos_rel, dev ^ j, axis=0, keepdims=False) for j in range(4)], axis=1)
        cos_t, sin_t = rope_tables(pos_mine)
        o01 = attention_call(qkv01, stats01, dev_arr, 0, 2, cos_t, sin_t, gain_q, gain_k)
        y_far01 = out_call([o01], (2, 3), x_far01, (2, 2), False, (2, 2), w_out, gain_out, gain_q)
        z_far01 = [swap(y_far01[0], 2), swap(y_far01[1], 3)]
        qkv2, stats2 = qkv_call(x_far2, (1, 1), False, weights, per_dev, 1, 2, (qkv01, stats01), y_far01[0])
        o2 = attention_call(qkv2, stats2, dev_arr, 2, 1, cos_t, sin_t, gain_q, gain_k)
        y_far2 = out_call([o2], (2, 3), x_far2, (1, 1), False, (1, 1), w_out, gain_out, gain_q)
        z_far2 = [swap(y_far2[0], 2), swap(y_far2[1], 3)]
        y_all, y_near = out_call([o01, o2], (0, 1), [x_loc, x_near], (per_dev, per_dev), True, (batch, per_dev), w_out, gain_out,
                                 y_far2[0], z_far01, ((2, 2, per_dev), (3, 2, per_dev)))
        z_near = swap(y_near, 1)

        def put(acc, part, r, first):
            return lax.dynamic_update_slice_in_dim(acc, part, (dev ^ r) * per_dev + first, axis=0)

        y_all = put(y_all, z_near, 1, 0)
        y_all = put(y_all, z_far2[0], 2, 2)
        y_all = put(y_all, z_far2[1], 3, 2)
        return y_all

    tok_spec = P('dp', 'sp', None)

    return jax.shard_map(local_block, mesh=mesh, in_specs=(tok_spec, P('dp', 'sp'), P(), P(), P(), P(), P(), P(), P()), out_specs=tok_spec, check_vma=False)
```

```python
import functools

import jax
import jax.numpy as jnp
from jax import lax
from jax.experimental import pallas as pl
from jax.experimental.pallas import tpu as pltpu
from jax.sharding import PartitionSpec as P


HEAD_DIM = 128
ROPE_THETA = 500000.0
NORM_EPS = 1e-6
SCALE = HEAD_DIM ** -0.5
LOG2E = 1.4426950408889634
QKV_TILE = 1280
OUT_TILE = 512
HEADS_PER_STEP = 4
VMEM_BYTES = 63 * 2 ** 20


def rope_tables(pos_ids):
    inv_freq = 1.0 / (ROPE_THETA ** (jnp.arange(0, HEAD_DIM, 2, dtype=jnp.float32) / HEAD_DIM))
    angles = pos_ids.astype(jnp.float32)[..., None] * inv_freq
    cos_t, sin_t = jnp.cos(angles), jnp.sin(angles)
    return cos_t, sin_t


def pair_heads(gain):
    return gain.reshape(-1, 2, 2, HEAD_DIM // 2).transpose(0, 2, 1, 3).reshape(1, -1)


def lane_sums(sq):
    part = sq[:, :128]
    for col in range(1, sq.shape[1] // 128):
        part = part + sq[:, col * 128:(col + 1) * 128]
    return part


def row_copies(srcs, dst, sems):
    return [pltpu.make_async_copy(src, dst.at[pl.ds(i * 128, 128), :], sems.at[i]) for i, src in enumerate(srcs)]


def pick_kernel(takes, per_dev, x_ref, *refs):
    outs, (buf, sem_in, sem_out) = refs[:len(takes)], refs[len(takes):]
    dev = lax.axis_index('sp')
    loads, stores = [], []
    for (r, first, count), out in zip(takes, outs):
        base = jnp.bitwise_xor(dev, r) * per_dev + first
        for b in range(count):
            i = len(loads)
            loads.append(pltpu.make_async_copy(x_ref.at[base + b], buf.at[i], sem_in.at[i]))
            stores.append(pltpu.make_async_copy(buf.at[i], out.at[b], sem_out.at[i]))
    for cp in loads:
        cp.start()
    for load, store in zip(loads, stores):
        load.wait()
        store.start()
    for cp in stores:
        cp.wait()


def pick_call(x_loc, takes, per_dev):
    n_total = sum(t[2] for t in takes)
    any_spec = pl.BlockSpec(memory_space=pl.ANY)
    return pl.pallas_call(
        functools.partial(pick_kernel, takes, per_dev),
        in_specs=[any_spec],
        out_specs=[any_spec] * len(takes),
        out_shape=[jax.ShapeDtypeStruct((t[2],) + x_loc.shape[1:], x_loc.dtype) for t in takes],
        scratch_shapes=[pltpu.VMEM((n_total,) + x_loc.shape[1:], x_loc.dtype)] + [pltpu.SemaphoreType.DMA((n_total,))] * 2,
        compiler_params=pltpu.CompilerParams(vmem_limit_bytes=VMEM_BYTES),
    )(x_loc)


def qkv_kernel(n_tiles, own, counts, aliased, *refs):
    n_pieces = len(counts)
    x_hbm = refs[:n_pieces]
    weights = refs[n_pieces:n_pieces + 3]
    qkv_out, stat_out, x_buf, w_buf, x_sem, w_sem = refs[n_pieces + 4 + 2 * aliased:]
    step = pl.program_id(0)
    rows = sum(counts) * 128
    slot = lax.rem(step, 2)

    def fetch(at_step):
        for idx, w_ref in enumerate(weights):
            @pl.when(at_step // n_tiles == idx)
            def _():
                cols = pl.ds(pl.multiple_of(lax.rem(at_step, n_tiles) * QKV_TILE, QKV_TILE), QKV_TILE)
                to = lax.rem(at_step, 2)
                pltpu.make_async_copy(w_ref.at[:, cols], w_buf.at[to], w_sem.at[to]).start()

    @pl.when(step == 0)
    def _():
        srcs = []
        for idx, (ref, count) in enumerate(zip(x_hbm, counts)):
            base = lax.axis_index('sp') * count if own and idx == 0 else 0
            srcs += [ref.at[base + b] for b in range(count)]
        copies = row_copies(srcs, x_buf, x_sem)
        for cp in copies:
            cp.start()
        fetch(step)
        for cp in copies:
            cp.wait()

    @pl.when(step + 1 < 3 * n_tiles)
    def _():
        fetch(step + 1)

    pltpu.make_async_copy(weights[0].at[:, pl.ds(0, QKV_TILE)], w_buf.at[slot], w_sem.at[slot]).wait()
    proj = jnp.dot(x_buf[...], w_buf[slot], preferred_element_type=jnp.float32)
    plain = step >= 2 * n_tiles
    low = lax.broadcasted_iota(jnp.int32, (rows, 128), 1) < 64
    keep_even = jnp.logical_or(low, plain)
    keep_odd = jnp.logical_not(jnp.logical_and(low, jnp.logical_not(plain)))
    part = None
    for pair in range(QKV_TILE // 256):
        cols = slice(pair * 256, pair * 256 + 128), slice(pair * 256 + 128, pair * 256 + 256)
        even, odd = (proj[:, c].astype(jnp.bfloat16) for c in cols)
        moved = pltpu.roll(jnp.where(low, odd, even), 64, 1)
        for c, val in zip(cols, (jnp.where(keep_even, even, moved), jnp.where(keep_odd, odd, moved))):
            qkv_out[0, :, :, :, c] = val.reshape(qkv_out.shape[1:4] + (128,))
        even, odd = even.astype(jnp.float32), odd.astype(jnp.float32)
        sq = even * even + odd * odd
        part = sq if part is None else part + sq
    part = part.reshape(stat_out.shape)
    first = lax.rem(step, n_tiles) == 0

    @pl.when(first)
    def _():
        stat_out[...] = part

    @pl.when(jnp.logical_not(first))
    def _():
        stat_out[...] = stat_out[...] + part


def qkv_call(pieces, counts, own, weights, per_dev, group, batch_block, prior, after):
    width = weights[0].shape[0]
    n_tiles = width // QKV_TILE
    n_batch = sum(counts) // 2
    rows = sum(counts) * 128
    any_spec = pl.BlockSpec(memory_space=pl.ANY)
    n_in = len(pieces) + 4
    return pl.pallas_call(
        functools.partial(qkv_kernel, n_tiles, own, counts, bool(prior)),
        grid=(3 * n_tiles,),
        in_specs=[any_spec] * (n_in + len(prior)),
        out_specs=[
            pl.BlockSpec((1, 2, n_batch, 128, QKV_TILE), lambda s: (s // n_tiles, group, batch_block, 0, lax.rem(s, n_tiles))),
            pl.BlockSpec((1, 2, n_batch, 128, 128), lambda s: (s // n_tiles, group, batch_block, 0, 0))],
        out_shape=[jax.ShapeDtypeStruct((3, 4, per_dev, 128, width), jnp.bfloat16),
                   jax.ShapeDtypeStruct((3, 4, per_dev, 128, 128), jnp.float32)],
        input_output_aliases={n_in: 0, n_in + 1: 1} if prior else {},
        scratch_shapes=[pltpu.VMEM((rows, width), jnp.bfloat16), pltpu.VMEM((2, width, QKV_TILE), jnp.bfloat16),
                        pltpu.SemaphoreType.DMA((sum(counts),)), pltpu.SemaphoreType.DMA((2,))],
        compiler_params=pltpu.CompilerParams(vmem_limit_bytes=VMEM_BYTES, dimension_semantics=("arbitrary",)),
        cost_estimate=pl.CostEstimate(flops=6 * rows * width * width, transcendentals=0, bytes_accessed=6 * width * width),
    )(*pieces, *weights, after, *prior)


def attention_kernel(width, dev_ref, *refs):
    qkv_refs, stat_refs = refs[:4], refs[4:8]
    cos_ref, sin_ref, gq_ref, gk_ref, out_ref, cos_n, sin_n = refs[8:]
    dev = dev_ref[0]

    @pl.when(pl.program_id(1) == 0)
    def _():
        for which in range(2):
            for j in range(4):
                rows = slice(j * 128, (j + 1) * 128)
                total = jnp.sum(stat_refs[j][which, 0, 0], axis=-1, keepdims=True)
                inv = lax.rsqrt(total * (1.0 / width) + NORM_EPS)
                cos_v, sin_v = cos_ref[0, rows, :], sin_ref[0, rows, :]
                cos_n[which, rows, :] = jnp.concatenate([cos_v, cos_v], axis=1) * inv
                sin_n[which, rows, :] = jnp.concatenate([sin_v, sin_v], axis=1) * inv

    row_id = lax.broadcasted_iota(jnp.int32, (128, 128), 0)
    col_id = lax.broadcasted_iota(jnp.int32, (128, 128), 1)
    causal = col_id <= row_id
    factor = SCALE * LOG2E
    zeros = jnp.zeros((128, 128), jnp.bfloat16)

    def scores(q, k):
        return lax.dot_general(q, k, (((1,), (1,)), ((), ())), preferred_element_type=jnp.float32)

    low = lax.broadcasted_iota(jnp.int32, (512, 128), 1) < 64
    nothing = jnp.zeros((512, 128), jnp.bfloat16)

    def prepare(pair):
        sides = []
        for which, gain_ref in ((0, gq_ref), (1, gk_ref)):
            halves = []
            for half in range(2):
                lanes = slice(pair * 256 + half * 128, pair * 256 + half * 128 + 128)
                gain = gain_ref[:, lanes].astype(jnp.float32)
                halves.append([qkv_refs[j][which, 0, 0, :, lanes].astype(jnp.float32) * gain for j in range(4)])
            rot = ([], [])
            for j in range(4):
                rows = slice(j * 128, (j + 1) * 128)
                cos_v, sin_v = cos_n[which, rows, :], sin_n[which, rows, :]
                first, second = halves[0][j], halves[1][j]
                rot[0].append((first * cos_v - second * sin_v).astype(jnp.bfloat16))
                rot[1].append((second * cos_v + first * sin_v).astype(jnp.bfloat16))
            sides.append([jnp.concatenate(r, axis=0) for r in rot])
        q = jnp.concatenate(sides[0], axis=1)
        out = []
        for head in range(2):
            k = jnp.concatenate([jnp.where(low, k_half, nothing) if head == 0 else jnp.where(low, nothing, k_half)
                                 for k_half in sides[1]], axis=1)
            out.append((scores(q, k[:256]), scores(q[256:], k[256:])))
        return out

    def finish(h, s_lo, s_hi):
        lanes = slice(h * 128, (h + 1) * 128)
        probs = []
        for j in range(4):
            blocks = []
            for c in range(j + 1):
                src, r = (s_lo, j) if c < 2 else (s_hi, j - 2)
                blk = src[r * 128:(r + 1) * 128, (c % 2) * 128:(c % 2 + 1) * 128]
                blocks.append(jnp.where(causal, blk, -1e30) if c == j else blk)
            top = functools.reduce(jnp.maximum, blocks)
            top = jnp.max(top, axis=-1, keepdims=True) * factor
            exps = [jnp.exp2(blk * factor - top) for blk in blocks]
            inv = 1.0 / jnp.sum(functools.reduce(jnp.add, exps), axis=-1, keepdims=True)
            row = [(e * inv).astype(jnp.bfloat16) for e in exps]
            probs.append(row + [zeros] * (4 - len(row)))
        p_lo = jnp.concatenate([jnp.concatenate(p[:2], axis=1) for p in probs], axis=0)
        p_hi = jnp.concatenate([jnp.concatenate(p[2:], axis=1) for p in probs[2:]], axis=0)
        v = [qkv_refs[j][2, 0, 0, :, lanes] for j in range(4)]
        o_lo = jnp.dot(p_lo, jnp.concatenate(v[:2], axis=0), preferred_element_type=jnp.float32)
        o_hi = jnp.dot(p_hi, jnp.concatenate(v[2:], axis=0), preferred_element_type=jnp.float32)
        for j in range(4):
            o = o_lo[j * 128:(j + 1) * 128]
            if j >= 2:
                o = o + o_hi[(j - 2) * 128:(j - 1) * 128]
            out_ref[jnp.bitwise_xor(dev, j), 0, :, lanes] = o.astype(jnp.bfloat16)

    ready = prepare(0)
    for pair in range(HEADS_PER_STEP // 2):
        following = prepare(pair + 1) if pair + 1 < HEADS_PER_STEP // 2 else None
        for head in range(2):
            finish(2 * pair + head, *ready[head])
        ready = following


def attention_call(qkv, stats, dev, first, n_batch, cos_t, sin_t, gain_q, gain_k):
    width = qkv.shape[-1]
    cols = HEADS_PER_STEP * 128

    def qkv_map(j):
        return lambda b, h, dev_ref: (0, jnp.bitwise_xor(dev_ref[0], j), b + first, 0, h)

    def stat_map(j):
        return lambda b, h, dev_ref: (0, jnp.bitwise_xor(dev_ref[0], j), b + first, 0, 0)

    table_spec = pl.BlockSpec((1, 512, HEAD_DIM // 2), lambda b, h, dev_ref: (b + first, 0, 0))
    gain_spec = pl.BlockSpec((1, cols), lambda b, h, dev_ref: (0, h))
    n_heads = width // 128
    return pl.pallas_call(
        functools.partial(attention_kernel, width),
        grid_spec=pltpu.PrefetchScalarGridSpec(
            num_scalar_prefetch=1,
            grid=(n_batch, width // cols),
            in_specs=[pl.BlockSpec((3, 1, 1, 128, cols), qkv_map(j)) for j in range(4)]
            + [pl.BlockSpec((2, 1, 1, 128, 128), stat_map(j)) for j in range(4)] + [table_spec] * 2 + [gain_spec] * 2,
            out_specs=pl.BlockSpec((4, 1, 128, cols), lambda b, h, dev_ref: (0, b, 0, h)),
            scratch_shapes=[pltpu.VMEM((2, 512, 128), jnp.float32)] * 2,
        ),
        out_shape=jax.ShapeDtypeStruct((4, n_batch, 128, width), jnp.bfloat16),
        compiler_params=pltpu.CompilerParams(vmem_limit_bytes=VMEM_BYTES, dimension_semantics=("arbitrary", "arbitrary")),
        cost_estimate=pl.CostEstimate(flops=n_batch * n_heads * 512 * 512 * 128 * 8, transcendentals=0,
                                      bytes_accessed=n_batch * 512 * width * 8),
    )(dev, *[qkv] * 4, *[stats] * 4, cos_t, sin_t, pair_heads(gain_q), pair_heads(gain_k))


def out_kernel(n_tiles, rel, o_counts, x_counts, own, moved, *refs):
    n_o, n_x, n_z = len(o_counts), len(x_counts), len(moved)
    pos = 0

    def take(n):
        nonlocal pos
        pos += n
        return refs[pos - n:pos]

    o_hbm, x_hbm, z_hbm = take(n_o), take(n_x), take(n_z)
    w_hbm, gain_ref, _ = take(3)
    y_hbm = take(n_x)
    o_buf, x_buf, a_buf, ss_buf, w_buf, o_sem, x_sem, y_sem, w_sem = take(9)
    z_buf, z_sem = take(2) if n_z else (None, None)
    step = pl.program_id(0)
    width = o_buf.shape[1]
    slot = lax.rem(step, 2)
    dev = lax.axis_index('sp')

    def fetch(at_step):
        cols = pl.ds(pl.multiple_of(at_step * OUT_TILE, OUT_TILE), OUT_TILE)
        to = lax.rem(at_step, 2)
        return pltpu.make_async_copy(w_hbm.at[:, cols], w_buf.at[to], w_sem.at[to])

    def at_pieces(piece_refs):
        out = []
        for idx, (ref, count) in enumerate(zip(piece_refs, x_counts)):
            base = dev * count if own and idx == 0 else 0
            out += [ref.at[base + b] for b in range(count)]
        return out

    def z_copies(outward):
        copies, i = [], 0
        for ref, (r, count, per_dev) in zip(z_hbm, moved):
            base = jnp.bitwise_xor(dev, r) * per_dev
            for b in range(count):
                src, dst = (z_buf.at[i], y_hbm[0].at[base + b]) if outward else (ref.at[b], z_buf.at[i])
                copies.append(pltpu.make_async_copy(src, dst, z_sem.at[int(outward), i]))
                i += 1
        return copies

    @pl.when(step == 0)
    def _():
        fetch(step).start()
        srcs = [ref.at[r, b] for r in rel for ref, count in zip(o_hbm, o_counts) for b in range(count)]
        copies = row_copies(srcs, o_buf, o_sem)
        for cp in copies:
            cp.start()
        for cp in copies:
            cp.wait()
        for cp in row_copies(at_pieces(x_hbm), x_buf, x_sem):
            cp.start()

    @pl.when(step + 1 < n_tiles)
    def _():
        fetch(step + 1).start()

    if n_z:
        @pl.when(step == 1)
        def _():
            for cp in z_copies(False):
                cp.start()

        @pl.when(step == 3)
        def _():
            for cp in z_copies(False):
                cp.wait()
            for cp in z_copies(True):
                cp.start()

    fetch(step).wait()
    a_tile = jnp.dot(o_buf[...], w_buf[slot], preferred_element_type=jnp.float32).astype(jnp.bfloat16)
    a_buf[step] = a_tile
    wide = a_tile.astype(jnp.float32)
    part = lane_sums(wide * wide)

    @pl.when(step == 0)
    def _():
        ss_buf[...] = part

    @pl.when(step != 0)
    def _():
        ss_buf[...] = ss_buf[...] + part

    @pl.when(step == n_tiles - 1)
    def _():
        for cp in row_copies(at_pieces(x_hbm), x_buf, x_sem):
            cp.wait()
        copies = []
        for i, dst in enumerate(at_pieces(y_hbm)):
            rows = slice(i * 128, (i + 1) * 128)
            inv = lax.rsqrt(jnp.sum(ss_buf[rows, :], axis=-1, keepdims=True) * (1.0 / width) + NORM_EPS)
            for t in range(n_tiles):
                cols = slice(t * OUT_TILE, (t + 1) * OUT_TILE)
                normed = a_buf[t, rows, :].astype(jnp.float32) * inv * gain_ref[:, cols].astype(jnp.float32)
                x_buf[rows, cols] = (x_buf[rows, cols].astype(jnp.float32) + normed).astype(jnp.bfloat16)
            cp = pltpu.make_async_copy(x_buf.at[pl.ds(i * 128, 128), :], dst, y_sem.at[i])
            cp.start()
            copies.append(cp)
        for cp in copies:
            cp.wait()
        if n_z:
            for cp in z_copies(True):
                cp.wait()


def out_call(o_list, rel, x_list, x_counts, own, out_batches, w_out, gain_out, after, z_list=(), moved=()):
    width = w_out.shape[0]
    n_tiles = width // OUT_TILE
    o_counts = tuple(o.shape[1] for o in o_list)
    rows = sum(x_counts) * 128
    any_spec = pl.BlockSpec(memory_space=pl.ANY)
    n_moved = sum(m[1] for m in moved)
    extra = [pltpu.VMEM((n_moved, 128, width), jnp.bfloat16), pltpu.SemaphoreType.DMA((2, n_moved))] if moved else []
    return pl.pallas_call(
        functools.partial(out_kernel, n_tiles, rel, o_counts, x_counts, own, moved),
        grid=(n_tiles,),
        in_specs=[any_spec] * (len(o_list) + len(x_list) + len(z_list) + 1)
        + [pl.BlockSpec((1, width), lambda step: (0, 0)), any_spec],
        out_specs=[any_spec] * len(x_list),
        out_shape=[jax.ShapeDtypeStruct((n, 128, width), jnp.bfloat16) for n in out_batches],
        scratch_shapes=[pltpu.VMEM((rows, width), jnp.bfloat16), pltpu.VMEM((rows, width), jnp.bfloat16),
                        pltpu.VMEM((n_tiles, rows, OUT_TILE), jnp.bfloat16), pltpu.VMEM((rows, 128), jnp.float32),
                        pltpu.VMEM((2, width, OUT_TILE), jnp.bfloat16)]
        + [pltpu.SemaphoreType.DMA((rows // 128,))] * 3 + [pltpu.SemaphoreType.DMA((2,))] + extra,
        compiler_params=pltpu.CompilerParams(vmem_limit_bytes=VMEM_BYTES, dimension_semantics=("arbitrary",)),
        cost_estimate=pl.CostEstimate(flops=2 * rows * width * width, transcendentals=0, bytes_accessed=2 * width * width),
    )(*o_list, *x_list, *z_list, w_out, gain_out.reshape(1, width), after)


def solution(mesh):
    def local_block(x_loc, pos_loc, w_query, w_key, w_value, w_out, gain_q, gain_k, gain_out):
        batch, _, _ = x_loc.shape
        per_dev = batch // 4
        dev = lax.axis_index('sp')

        def swap(arr, r):
            return lax.ppermute(arr, 'sp', [(i, i ^ r) for i in range(4)])

        for_near, = pick_call(x_loc, ((1, 0, per_dev),), per_dev)
        x_near = swap(for_near, 1)
        p01_2, p01_3, p2, p3 = pick_call(x_loc, ((2, 0, 2), (3, 0, 2), (2, 2, 1), (3, 2, 1)), per_dev)
        x_far01 = [swap(p01_2, 2), swap(p01_3, 3)]
        pos_parts = [lax.dynamic_slice_in_dim(pos_loc, dev * per_dev, per_dev, axis=0)]
        for r in range(1, 4):
            pos_parts.append(swap(lax.dynamic_slice_in_dim(pos_loc, (dev ^ r) * per_dev, per_dev, axis=0), r))

        weights = (w_query, w_key, w_value)
        dev_arr = jnp.full((1,), dev, jnp.int32)
        near = qkv_call([x_loc, x_near], (per_dev, per_dev), True, weights, per_dev, 0, 0, (), gain_q)
        p2, p3, x_far01[0], x_far01[1] = lax.optimization_barrier((p2, p3, x_far01[0], x_far01[1]))
        x_far2 = [swap(p2, 2), swap(p3, 3)]
        qkv01, stats01 = qkv_call(x_far01, (2, 2), False, weights, per_dev, 1, 0, near, gain_q)
        pos_parts, _ = lax.optimization_barrier((pos_parts, near[1]))
        pos_rel = jnp.stack(pos_parts)
        pos_mine = jnp.concatenate([lax.dynamic_index_in_dim(pos_rel, dev ^ j, axis=0, keepdims=False) for j in range(4)], axis=1)
        cos_t, sin_t = rope_tables(pos_mine)
        o01 = attention_call(qkv01, stats01, dev_arr, 0, 2, cos_t, sin_t, gain_q, gain_k)
        y_far01 = out_call([o01], (2, 3), x_far01, (2, 2), False, (2, 2), w_out, gain_out, gain_q)
        z_far01 = [swap(y_far01[0], 2), swap(y_far01[1], 3)]
        qkv2, stats2 = qkv_call(x_far2, (1, 1), False, weights, per_dev, 1, 2, (qkv01, stats01), y_far01[0])
        o2 = attention_call(qkv2, stats2, dev_arr, 2, 1, cos_t, sin_t, gain_q, gain_k)
        y_far2 = out_call([o2], (2, 3), x_far2, (1, 1), False, (1, 1), w_out, gain_out, gain_q)
        z_far2 = [swap(y_far2[0], 2), swap(y_far2[1], 3)]
        y_all, y_near = out_call([o01, o2], (0, 1), [x_loc, x_near], (per_dev, per_dev), True, (batch, per_dev), w_out, gain_out,
                                 y_far2[0], z_far01, ((2, 2, per_dev), (3, 2, per_dev)))
        z_near = swap(y_near, 1)

        def put(acc, part, r, first):
            return lax.dynamic_update_slice_in_dim(acc, part, (dev ^ r) * per_dev + first, axis=0)

        y_all = put(y_all, z_far2[0], 2, 2)
        y_all = put(y_all, z_far2[1], 3, 2)
        y_all = put(y_all, z_near, 1, 0)
        return y_all

    tok_spec = P('dp', 'sp', None)

    return jax.shard_map(local_block, mesh=mesh, in_specs=(tok_spec, P('dp', 'sp'), P(), P(), P(), P(), P(), P(), P()), out_specs=tok_spec, check_vma=False)
```

```python
import functools

import jax
import jax.numpy as jnp
from jax import lax
from jax.experimental import pallas as pl
from jax.experimental.pallas import tpu as pltpu
from jax.sharding import PartitionSpec as P


HEAD_DIM = 128
ROPE_THETA = 500000.0
NORM_EPS = 1e-6
SCALE = HEAD_DIM ** -0.5
LOG2E = 1.4426950408889634
QKV_TILE = 1280
OUT_TILE = 512
HEADS_PER_STEP = 4
VMEM_BYTES = 63 * 2 ** 20


def rope_tables(pos_ids):
    inv_freq = 1.0 / (ROPE_THETA ** (jnp.arange(0, HEAD_DIM, 2, dtype=jnp.float32) / HEAD_DIM))
    angles = pos_ids.astype(jnp.float32)[..., None] * inv_freq
    cos_t, sin_t = jnp.cos(angles), jnp.sin(angles)
    return cos_t, sin_t


def lane_sums(sq):
    part = sq[:, :128]
    for col in range(1, sq.shape[1] // 128):
        part = part + sq[:, col * 128:(col + 1) * 128]
    return part


def row_copies(srcs, dst, sems):
    return [pltpu.make_async_copy(src, dst.at[pl.ds(i * 128, 128), :], sems.at[i]) for i, src in enumerate(srcs)]


def pick_kernel(takes, per_dev, x_ref, *refs):
    outs, (buf, sem_in, sem_out) = refs[:len(takes)], refs[len(takes):]
    dev = lax.axis_index('sp')
    loads, stores = [], []
    for (r, first, count), out in zip(takes, outs):
        base = jnp.bitwise_xor(dev, r) * per_dev + first
        for b in range(count):
            i = len(loads)
            loads.append(pltpu.make_async_copy(x_ref.at[base + b], buf.at[i], sem_in.at[i]))
            stores.append(pltpu.make_async_copy(buf.at[i], out.at[b], sem_out.at[i]))
    for cp in loads:
        cp.start()
    for load, store in zip(loads, stores):
        load.wait()
        store.start()
    for cp in stores:
        cp.wait()


def pick_call(x_loc, takes, per_dev):
    n_total = sum(t[2] for t in takes)
    any_spec = pl.BlockSpec(memory_space=pl.ANY)
    return pl.pallas_call(
        functools.partial(pick_kernel, takes, per_dev),
        in_specs=[any_spec],
        out_specs=[any_spec] * len(takes),
        out_shape=[jax.ShapeDtypeStruct((t[2],) + x_loc.shape[1:], x_loc.dtype) for t in takes],
        scratch_shapes=[pltpu.VMEM((n_total,) + x_loc.shape[1:], x_loc.dtype)] + [pltpu.SemaphoreType.DMA((n_total,))] * 2,
        compiler_params=pltpu.CompilerParams(vmem_limit_bytes=VMEM_BYTES),
    )(x_loc)


def qkv_kernel(n_tiles, n_arrays, takes, aliased, *refs):
    arrays = refs[:n_arrays]
    weights = refs[n_arrays:n_arrays + 3]
    qkv_out, stat_out, x_buf, w_buf, o_buf, stat_buf, x_sem, w_sem, o_sem, stat_sem = refs[n_arrays + 4 + 2 * aliased:]
    step = pl.program_id(0)
    rows = x_buf.shape[0]
    slot = lax.rem(step, 2)
    which = step // n_tiles
    srcs, spots = [], []
    for idx, own, first, count, rel, batch in takes:
        base = lax.axis_index('sp') * count if own else first
        srcs += [arrays[idx].at[base + b] for b in range(count)]
        spots += [(rel, batch + b) for b in range(count)]

    def result_copies(at_step):
        cols = pl.ds(pl.multiple_of(lax.rem(at_step, n_tiles) * QKV_TILE, QKV_TILE), QKV_TILE)
        frm = lax.rem(at_step, 2)
        return [pltpu.make_async_copy(o_buf.at[frm, pl.ds(i * 128, 128), :], qkv_out.at[at_step // n_tiles, rel, b, :, cols],
                                      o_sem.at[frm, i]) for i, (rel, b) in enumerate(spots)]

    @pl.when(step >= 2)
    def _():
        for cp in result_copies(step - 2):
            cp.wait()

    def fetch(at_step):
        for idx, w_ref in enumerate(weights):
            @pl.when(at_step // n_tiles == idx)
            def _():
                cols = pl.ds(pl.multiple_of(lax.rem(at_step, n_tiles) * QKV_TILE, QKV_TILE), QKV_TILE)
                to = lax.rem(at_step, 2)
                pltpu.make_async_copy(w_ref.at[:, cols], w_buf.at[to], w_sem.at[to]).start()

    @pl.when(step == 0)
    def _():
        copies = row_copies(srcs, x_buf, x_sem)
        for cp in copies:
            cp.start()
        fetch(step)
        for cp in copies:
            cp.wait()

    @pl.when(step + 1 < 3 * n_tiles)
    def _():
        fetch(step + 1)

    pltpu.make_async_copy(weights[0].at[:, pl.ds(0, QKV_TILE)], w_buf.at[slot], w_sem.at[slot]).wait()
    proj = jnp.dot(x_buf[...], w_buf[slot], preferred_element_type=jnp.float32)
    plain = step >= 2 * n_tiles
    low = lax.broadcasted_iota(jnp.int32, (rows, 128), 1) < 64
    keep_even = jnp.logical_or(low, plain)
    keep_odd = jnp.logical_not(jnp.logical_and(low, jnp.logical_not(plain)))
    part = None
    for pair in range(QKV_TILE // 256):
        cols = slice(pair * 256, pair * 256 + 128), slice(pair * 256 + 128, pair * 256 + 256)
        even, odd = (proj[:, c].astype(jnp.bfloat16) for c in cols)
        moved = pltpu.roll(jnp.where(low, odd, even), 64, 1)
        for c, val in zip(cols, (jnp.where(keep_even, even, moved), jnp.where(keep_odd, odd, moved))):
            o_buf[slot, :, c] = val
        even, odd = even.astype(jnp.float32), odd.astype(jnp.float32)
        sq = even * even + odd * odd
        part = sq if part is None else part + sq
    for cp in result_copies(step):
        cp.start()
    first = lax.rem(step, n_tiles) == 0

    @pl.when(first)
    def _():
        stat_buf[which] = part

    @pl.when(jnp.logical_not(first))
    def _():
        stat_buf[which] = stat_buf[which] + part

    @pl.when(step == 3 * n_tiles - 1)
    def _():
        copies = [pltpu.make_async_copy(stat_buf.at[w, pl.ds(i * 128, 128), :], stat_out.at[w, rel, b], stat_sem.at[w, i])
                  for w in range(3) for i, (rel, b) in enumerate(spots)]
        for cp in copies:
            cp.start()
        for cp in result_copies(step - 1) + result_copies(step) + copies:
            cp.wait()


def qkv_call(arrays, takes, weights, per_dev, prior, after):
    width = weights[0].shape[0]
    n_tiles = width // QKV_TILE
    n_rows = sum(t[3] for t in takes)
    rows = n_rows * 128
    any_spec = pl.BlockSpec(memory_space=pl.ANY)
    n_in = len(arrays) + 4
    return pl.pallas_call(
        functools.partial(qkv_kernel, n_tiles, len(arrays), takes, bool(prior)),
        grid=(3 * n_tiles,),
        in_specs=[any_spec] * (n_in + len(prior)),
        out_specs=[any_spec] * 2,
        out_shape=[jax.ShapeDtypeStruct((3, 4, per_dev, 128, width), jnp.bfloat16),
                   jax.ShapeDtypeStruct((3, 4, per_dev, 128, 128), jnp.float32)],
        input_output_aliases={n_in: 0, n_in + 1: 1} if prior else {},
        scratch_shapes=[pltpu.VMEM((rows, width), jnp.bfloat16), pltpu.VMEM((2, width, QKV_TILE), jnp.bfloat16),
                        pltpu.VMEM((2, rows, QKV_TILE), jnp.bfloat16), pltpu.VMEM((3, rows, 128), jnp.float32),
                        pltpu.SemaphoreType.DMA((n_rows,)), pltpu.SemaphoreType.DMA((2,)),
                        pltpu.SemaphoreType.DMA((2, n_rows)), pltpu.SemaphoreType.DMA((3, n_rows))],
        compiler_params=pltpu.CompilerParams(vmem_limit_bytes=VMEM_BYTES, dimension_semantics=("arbitrary",)),
        cost_estimate=pl.CostEstimate(flops=6 * rows * width * width, transcendentals=0, bytes_accessed=6 * width * width),
    )(*arrays, *weights, after, *prior)


def attention_kernel(width, dev_ref, *refs):
    qkv_refs, stat_refs = refs[:4], refs[4:8]
    cos_ref, sin_ref, gq_ref, gk_ref, out_ref, cos_n, sin_n = refs[8:]
    dev = dev_ref[0]

    @pl.when(pl.program_id(1) == 0)
    def _():
        for which in range(2):
            for j in range(4):
                rows = slice(j * 128, (j + 1) * 128)
                total = jnp.sum(stat_refs[j][which, 0, 0], axis=-1, keepdims=True)
                inv = lax.rsqrt(total * (1.0 / width) + NORM_EPS)
                cos_v, sin_v = cos_ref[0, rows, :], sin_ref[0, rows, :]
                cos_n[which, rows, :] = jnp.concatenate([cos_v, cos_v], axis=1) * inv
                sin_n[which, rows, :] = jnp.concatenate([sin_v, sin_v], axis=1) * inv

    row_id = lax.broadcasted_iota(jnp.int32, (128, 128), 0)
    col_id = lax.broadcasted_iota(jnp.int32, (128, 128), 1)
    causal = col_id <= row_id
    factor = SCALE * LOG2E
    zeros = jnp.zeros((128, 128), jnp.bfloat16)

    def scores(q, k):
        return lax.dot_general(q, k, (((1,), (1,)), ((), ())), preferred_element_type=jnp.float32)

    low = lax.broadcasted_iota(jnp.int32, (512, 128), 1) < 64
    nothing = jnp.zeros((512, 128), jnp.bfloat16)

    def prepare(pair):
        sides = []
        for which, gain_ref in ((0, gq_ref), (1, gk_ref)):
            halves = []
            even, odd = (gain_ref[:, pair * 256 + c:pair * 256 + c + 128].astype(jnp.float32) for c in (0, 128))
            moved = pltpu.roll(jnp.where(low[:1], odd, even), 64, 1)
            gains = jnp.where(low[:1], even, moved), jnp.where(low[:1], moved, odd)
            for half in range(2):
                lanes = slice(pair * 256 + half * 128, pair * 256 + half * 128 + 128)
                halves.append([qkv_refs[j][which, 0, 0, :, lanes].astype(jnp.float32) * gains[half] for j in range(4)])
            rot = ([], [])
            for j in range(4):
                rows = slice(j * 128, (j + 1) * 128)
                cos_v, sin_v = cos_n[which, rows, :], sin_n[which, rows, :]
                first, second = halves[0][j], halves[1][j]
                rot[0].append((first * cos_v - second * sin_v).astype(jnp.bfloat16))
                rot[1].append((second * cos_v + first * sin_v).astype(jnp.bfloat16))
            sides.append([jnp.concatenate(r, axis=0) for r in rot])
        q = jnp.concatenate(sides[0], axis=1)
        out = []
        for head in range(2):
            k = jnp.concatenate([jnp.where(low, k_half, nothing) if head == 0 else jnp.where(low, nothing, k_half)
                                 for k_half in sides[1]], axis=1)
            out.append((scores(q, k[:256]), scores(q[256:], k[256:])))
        return out

    def finish(h, s_lo, s_hi):
        lanes = slice(h * 128, (h + 1) * 128)
        probs = []
        for j in range(4):
            blocks = []
            for c in range(j + 1):
                src, r = (s_lo, j) if c < 2 else (s_hi, j - 2)
                blk = src[r * 128:(r + 1) * 128, (c % 2) * 128:(c % 2 + 1) * 128]
                blocks.append(jnp.where(causal, blk, -1e30) if c == j else blk)
            top = functools.reduce(jnp.maximum, blocks)
            top = jnp.max(top, axis=-1, keepdims=True) * factor
            exps = [jnp.exp2(blk * factor - top) for blk in blocks]
            inv = 1.0 / jnp.sum(functools.reduce(jnp.add, exps), axis=-1, keepdims=True)
            row = [(e * inv).astype(jnp.bfloat16) for e in exps]
            probs.append(row + [zeros] * (4 - len(row)))
        p_lo = jnp.concatenate([jnp.concatenate(p[:2], axis=1) for p in probs], axis=0)
        p_hi = jnp.concatenate([jnp.concatenate(p[2:], axis=1) for p in probs[2:]], axis=0)
        v = [qkv_refs[j][2, 0, 0, :, lanes] for j in range(4)]
        o_lo = jnp.dot(p_lo, jnp.concatenate(v[:2], axis=0), preferred_element_type=jnp.float32)
        o_hi = jnp.dot(p_hi, jnp.concatenate(v[2:], axis=0), preferred_element_type=jnp.float32)
        for j in range(4):
            o = o_lo[j * 128:(j + 1) * 128]
            if j >= 2:
                o = o + o_hi[(j - 2) * 128:(j - 1) * 128]
            out_ref[jnp.bitwise_xor(dev, j), 0, :, lanes] = o.astype(jnp.bfloat16)

    ready = prepare(0)
    for pair in range(HEADS_PER_STEP // 2):
        following = prepare(pair + 1) if pair + 1 < HEADS_PER_STEP // 2 else None
        for head in range(2):
            finish(2 * pair + head, *ready[head])
        ready = following


def attention_call(qkv, stats, dev, first, n_batch, cos_t, sin_t, gain_q, gain_k):
    width = qkv.shape[-1]
    cols = HEADS_PER_STEP * 128

    def qkv_map(j):
        return lambda b, h, dev_ref: (0, jnp.bitwise_xor(dev_ref[0], j), b + first, 0, h)

    def stat_map(j):
        return lambda b, h, dev_ref: (0, jnp.bitwise_xor(dev_ref[0], j), b + first, 0, 0)

    table_spec = pl.BlockSpec((1, 512, HEAD_DIM // 2), lambda b, h, dev_ref: (b + first, 0, 0))
    gain_spec = pl.BlockSpec((1, cols), lambda b, h, dev_ref: (0, h))
    n_heads = width // 128
    return pl.pallas_call(
        functools.partial(attention_kernel, width),
        grid_spec=pltpu.PrefetchScalarGridSpec(
            num_scalar_prefetch=1,
            grid=(n_batch, width // cols),
            in_specs=[pl.BlockSpec((3, 1, 1, 128, cols), qkv_map(j)) for j in range(4)]
            + [pl.BlockSpec((2, 1, 1, 128, 128), stat_map(j)) for j in range(4)] + [table_spec] * 2 + [gain_spec] * 2,
            out_specs=pl.BlockSpec((4, 1, 128, cols), lambda b, h, dev_ref: (0, b, 0, h)),
            scratch_shapes=[pltpu.VMEM((2, 512, 128), jnp.float32)] * 2,
        ),
        out_shape=jax.ShapeDtypeStruct((4, n_batch, 128, width), jnp.bfloat16),
        compiler_params=pltpu.CompilerParams(vmem_limit_bytes=VMEM_BYTES, dimension_semantics=("arbitrary", "arbitrary")),
        cost_estimate=pl.CostEstimate(flops=n_batch * n_heads * 512 * 512 * 128 * 8, transcendentals=0,
                                      bytes_accessed=n_batch * 512 * width * 8),
    )(dev, *[qkv] * 4, *[stats] * 4, cos_t, sin_t, gain_q.reshape(1, width), gain_k.reshape(1, width))


def out_kernel(n_tiles, rel, o_counts, x_counts, own, moved, *refs):
    n_o, n_x, n_z = len(o_counts), len(x_counts), len(moved)
    pos = 0

    def take(n):
        nonlocal pos
        pos += n
        return refs[pos - n:pos]

    o_hbm, x_hbm, z_hbm = take(n_o), take(n_x), take(n_z)
    w_hbm, gain_ref, _ = take(3)
    y_hbm = take(n_x)
    o_buf, x_buf, a_buf, ss_buf, w_buf, o_sem, x_sem, y_sem, w_sem = take(9)
    z_buf, z_sem = take(2) if n_z else (None, None)
    step = pl.program_id(0)
    width = o_buf.shape[1]
    slot = lax.rem(step, 2)
    dev = lax.axis_index('sp')

    def fetch(at_step):
        cols = pl.ds(pl.multiple_of(at_step * OUT_TILE, OUT_TILE), OUT_TILE)
        to = lax.rem(at_step, 2)
        return pltpu.make_async_copy(w_hbm.at[:, cols], w_buf.at[to], w_sem.at[to])

    def at_pieces(piece_refs):
        out = []
        for idx, (ref, count) in enumerate(zip(piece_refs, x_counts)):
            base = dev * count if own and idx == 0 else 0
            out += [ref.at[base + b] for b in range(count)]
        return out

    def z_copies(outward):
        copies, i = [], 0
        for ref, (r, count, per_dev) in zip(z_hbm, moved):
            base = jnp.bitwise_xor(dev, r) * per_dev
            for b in range(count):
                src, dst = (z_buf.at[i], y_hbm[0].at[base + b]) if outward else (ref.at[b], z_buf.at[i])
                copies.append(pltpu.make_async_copy(src, dst, z_sem.at[int(outward), i]))
                i += 1
        return copies

    @pl.when(step == 0)
    def _():
        fetch(step).start()
        srcs = [ref.at[r, b] for r in rel for ref, count in zip(o_hbm, o_counts) for b in range(count)]
        copies = row_copies(srcs, o_buf, o_sem)
        for cp in copies:
            cp.start()
        for cp in copies:
            cp.wait()
        for cp in row_copies(at_pieces(x_hbm), x_buf, x_sem):
            cp.start()

    @pl.when(step + 1 < n_tiles)
    def _():
        fetch(step + 1).start()

    if n_z:
        @pl.when(step == 1)
        def _():
            for cp in z_copies(False):
                cp.start()

        @pl.when(step == 3)
        def _():
            for cp in z_copies(False):
                cp.wait()
            for cp in z_copies(True):
                cp.start()

    fetch(step).wait()
    a_tile = jnp.dot(o_buf[...], w_buf[slot], preferred_element_type=jnp.float32).astype(jnp.bfloat16)
    a_buf[step] = a_tile
    wide = a_tile.astype(jnp.float32)
    part = lane_sums(wide * wide)

    @pl.when(step == 0)
    def _():
        ss_buf[...] = part

    @pl.when(step != 0)
    def _():
        ss_buf[...] = ss_buf[...] + part

    @pl.when(step == n_tiles - 1)
    def _():
        for cp in row_copies(at_pieces(x_hbm), x_buf, x_sem):
            cp.wait()
        copies = []
        for i, dst in enumerate(at_pieces(y_hbm)):
            rows = slice(i * 128, (i + 1) * 128)
            inv = lax.rsqrt(jnp.sum(ss_buf[rows, :], axis=-1, keepdims=True) * (1.0 / width) + NORM_EPS)
            for t in range(n_tiles):
                cols = slice(t * OUT_TILE, (t + 1) * OUT_TILE)
                normed = a_buf[t, rows, :].astype(jnp.float32) * inv * gain_ref[:, cols].astype(jnp.float32)
                x_buf[rows, cols] = (x_buf[rows, cols].astype(jnp.float32) + normed).astype(jnp.bfloat16)
            cp = pltpu.make_async_copy(x_buf.at[pl.ds(i * 128, 128), :], dst, y_sem.at[i])
            cp.start()
            copies.append(cp)
        for cp in copies:
            cp.wait()
        if n_z:
            for cp in z_copies(True):
                cp.wait()


def out_call(o_list, rel, x_list, x_counts, own, out_batches, w_out, gain_out, after, z_list=(), moved=()):
    width = w_out.shape[0]
    n_tiles = width // OUT_TILE
    o_counts = tuple(o.shape[1] for o in o_list)
    rows = sum(x_counts) * 128
    any_spec = pl.BlockSpec(memory_space=pl.ANY)
    n_moved = sum(m[1] for m in moved)
    extra = [pltpu.VMEM((n_moved, 128, width), jnp.bfloat16), pltpu.SemaphoreType.DMA((2, n_moved))] if moved else []
    return pl.pallas_call(
        functools.partial(out_kernel, n_tiles, rel, o_counts, x_counts, own, moved),
        grid=(n_tiles,),
        in_specs=[any_spec] * (len(o_list) + len(x_list) + len(z_list) + 1)
        + [pl.BlockSpec((1, width), lambda step: (0, 0)), any_spec],
        out_specs=[any_spec] * len(x_list),
        out_shape=[jax.ShapeDtypeStruct((n, 128, width), jnp.bfloat16) for n in out_batches],
        scratch_shapes=[pltpu.VMEM((rows, width), jnp.bfloat16), pltpu.VMEM((rows, width), jnp.bfloat16),
                        pltpu.VMEM((n_tiles, rows, OUT_TILE), jnp.bfloat16), pltpu.VMEM((rows, 128), jnp.float32),
                        pltpu.VMEM((2, width, OUT_TILE), jnp.bfloat16)]
        + [pltpu.SemaphoreType.DMA((rows // 128,))] * 3 + [pltpu.SemaphoreType.DMA((2,))] + extra,
        compiler_params=pltpu.CompilerParams(vmem_limit_bytes=VMEM_BYTES, dimension_semantics=("arbitrary",)),
        cost_estimate=pl.CostEstimate(flops=2 * rows * width * width, transcendentals=0, bytes_accessed=2 * width * width),
    )(*o_list, *x_list, *z_list, w_out, gain_out.reshape(1, width), after)


def solution(mesh):
    def local_block(x_loc, pos_loc, w_query, w_key, w_value, w_out, gain_q, gain_k, gain_out):
        batch, _, _ = x_loc.shape
        per_dev = batch // 4
        dev = lax.axis_index('sp')

        def swap(arr, r):
            return lax.ppermute(arr, 'sp', [(i, i ^ r) for i in range(4)])

        for_near, = pick_call(x_loc, ((1, 0, per_dev),), per_dev)
        x_near = swap(for_near, 1)
        p01_2, p01_3, p2, p3 = pick_call(x_loc, ((2, 0, 2), (3, 0, 2), (2, 2, 1), (3, 2, 1)), per_dev)
        x_far01 = [swap(p01_2, 2), swap(p01_3, 3)]
        pos_parts = [lax.dynamic_slice_in_dim(pos_loc, dev * per_dev, per_dev, axis=0)]
        for r in range(1, 4):
            pos_parts.append(swap(lax.dynamic_slice_in_dim(pos_loc, (dev ^ r) * per_dev, per_dev, axis=0), r))

        weights = (w_query, w_key, w_value)
        dev_arr = jnp.full((1,), dev, jnp.int32)
        near = qkv_call([x_loc, x_near], ((0, True, 0, per_dev, 0, 0), (1, False, 0, 2, 1, 0)), weights, per_dev, (), gain_q)
        p2, p3, x_far01[0], x_far01[1] = lax.optimization_barrier((p2, p3, x_far01[0], x_far01[1]))
        x_far2 = [swap(p2, 2), swap(p3, 3)]
        qkv01, stats01 = qkv_call(x_far01, ((0, False, 0, 2, 2, 0), (1, False, 0, 2, 3, 0)), weights, per_dev, near, gain_q)
        pos_parts, _ = lax.optimization_barrier((pos_parts, near[1]))
        pos_rel = jnp.stack(pos_parts)
        pos_mine = jnp.concatenate([lax.dynamic_index_in_dim(pos_rel, dev ^ j, axis=0, keepdims=False) for j in range(4)], axis=1)
        cos_t, sin_t = rope_tables(pos_mine)
        o01 = attention_call(qkv01, stats01, dev_arr, 0, 2, cos_t, sin_t, gain_q, gain_k)
        y_far01 = out_call([o01], (2, 3), x_far01, (2, 2), False, (2, 2), w_out, gain_out, gain_q)
        z_far01 = [swap(y_far01[0], 2), swap(y_far01[1], 3)]
        qkv2, stats2 = qkv_call([x_near] + x_far2, ((0, False, 2, 1, 1, 2), (1, False, 0, 1, 2, 2), (2, False, 0, 1, 3, 2)), weights, per_dev,
                                 (qkv01, stats01), y_far01[0])
        o2 = attention_call(qkv2, stats2, dev_arr, 2, 1, cos_t, sin_t, gain_q, gain_k)
        y_far2 = out_call([o2], (2, 3), x_far2, (1, 1), False, (1, 1), w_out, gain_out, gain_q)
        z_far2 = [swap(y_far2[0], 2), swap(y_far2[1], 3)]
        y_all, y_near = out_call([o01, o2], (0, 1), [x_loc, x_near], (per_dev, per_dev), True, (batch, per_dev), w_out, gain_out,
                                 y_far2[0], z_far01, ((2, 2, per_dev), (3, 2, per_dev)))
        z_near = swap(y_near, 1)

        def put(acc, part, r, first):
            return lax.dynamic_update_slice_in_dim(acc, part, (dev ^ r) * per_dev + first, axis=0)

        y_all = put(y_all, z_far2[0], 2, 2)
        y_all = put(y_all, z_far2[1], 3, 2)
        y_all = put(y_all, z_near, 1, 0)
        return y_all

    tok_spec = P('dp', 'sp', None)

    return jax.shard_map(local_block, mesh=mesh, in_specs=(tok_spec, P('dp', 'sp'), P(), P(), P(), P(), P(), P(), P()), out_specs=tok_spec, check_vma=False)
```
